512 devices in a mesh: seq: 128 (over x, z, core), head: 4 (over y).
Axes of the slice: x: 4, y: 4, z: 16, core: 2. Of those that a mesh axis runs over, the one named last changes fastest.
Arguments:
- q_raw: bfloat16 [65536, 4096], P('seq', 'head'), may hold values from -120 to 120
- k_raw: bfloat16 [65536, 4096], P('seq', 'head'), may hold values from -6 to 6
- v_raw: bfloat16 [65536, 4096], P('seq', 'head'), may hold values from -6 to 6
- block_scales: float32 [3, 512, 32], P(None, 'seq', 'head'), may hold values from 0.25 to 4
- segment_ids: int32 [65536], P('seq'), may hold values from 0 to 504, as said below
- norm_gain: float32 [4096], P('head'), may hold values from 0.5 to 1.5
Outputs:
- attended: bfloat16 [65536, 4096], P('seq', 'head')
The draws below stay inside these ranges and needn't reach their ends.
Inputs may be any that keep to these rules, and one draw needn't show every extreme that they name: `segment_ids`: ids start at 0 and never fall, rising by at most one from a token to the next. Each aligned block of 512 tokens has exactly 4 segment starts, except the second and third blocks, which have none; in the second-to-last block all starts lie in the block's first half, in the last block all lie in its second half. No segment starts at the first token of a block except segment 0 at token 0.
All inputs are finite; a program needn't handle non-finite values.
Results may differ from the reference program's by a relative error of at most 0.013.
Values may be sent and summed in bfloat16 or wider, within the bound.
A program may use at most 64 MiB of HBM per device.

```python
import math
import jax
import jax.numpy as jnp
from jax import lax

H = 32
HD = 128
TOK_DEV = 512
BLK = 128
CAP = 4
SEQ = 65536
N_SEQ = 128


def segment_draw(key):
    block_total = SEQ // TOK_DEV
    half_len = TOK_DEV // 2
    perm_key = jax.random.fold_in(key, 11)
    perm_keys = jax.random.split(perm_key, block_total)
    orders = jax.vmap(lambda subkey: jax.random.permutation(subkey, TOK_DEV - 1))(perm_keys).astype(jnp.int32)
    block_index = jnp.arange(block_total, dtype=jnp.int32)
    spots = jnp.arange(1, TOK_DEV, dtype=jnp.int32)
    last_block = (block_index == block_total - 1)[:, None]
    before_last = (block_index == block_total - 2)[:, None]
    early_spot = (spots < half_len)[None, :]
    pushed = last_block & early_spot | before_last & jnp.logical_not(early_spot)
    keyed = orders + jnp.where(pushed, TOK_DEV, 0).astype(jnp.int32)
    ranks = jnp.argsort(jnp.argsort(keyed, axis=1, stable=True), axis=1, stable=True)
    start_count = jnp.where((block_index == 1) | (block_index == 2), 0, CAP).astype(jnp.int32)
    flags = (ranks < start_count[:, None]).astype(jnp.int32)
    flags = jnp.concatenate([jnp.zeros((block_total, 1), jnp.int32), flags], axis=1).reshape(SEQ)
    return jnp.cumsum(flags).astype(jnp.int32)


def pair_draw(key):
    segment_index = segment_draw(key)
    base = jax.random.fold_in(key, 7)
    query_key, key_key, shared_key = jax.random.split(base, 3)
    shared_table = 0.7 * jax.random.normal(shared_key, (CAP * (SEQ // TOK_DEV) + 1, H * HD), jnp.float32)
    common = shared_table[segment_index]
    keys_drawn = jnp.clip(jax.random.normal(key_key, (SEQ, H * HD), jnp.float32) + common, -6.0, 6.0)
    queries_drawn = jnp.clip(jax.random.normal(query_key, (SEQ, H * HD), jnp.float32) + common, -6.0, 6.0)
    return (queries_drawn, keys_drawn)


def draw_k_raw(key, part):
    return pair_draw(key)[1].astype(jnp.bfloat16)


def draw_q_raw(key, part):
    queries_drawn, keys_drawn = pair_draw(key)
    return queries_drawn.astype(jnp.bfloat16)


def draw_v_raw(key, part):
    base = jax.random.fold_in(key, 13)
    noise_key, offset_key = jax.random.split(base)
    offsets = 0.8 * jax.random.normal(offset_key, (SEQ // BLK, H * HD), jnp.float32)
    values_drawn = jax.random.normal(noise_key, (SEQ, H * HD), jnp.float32) + jnp.repeat(offsets, BLK, axis=0)
    return jnp.clip(values_drawn, -6.0, 6.0).astype(jnp.bfloat16)


def draw_segment_ids(key, part):
    return segment_draw(key)


def level_of(own_key, extent, cuts, least, high):
    level, own = 1.0, jax.random.fold_in(own_key, 6)
    for position, shards_of in cuts:
        draws = jnp.exp(jax.random.uniform(jax.random.fold_in(own, position), (shards_of,), jnp.float32, least / len(cuts), high / len(cuts)))
        level = level * jnp.repeat(draws, extent[position] // shards_of).reshape([-1 if axis == position else 1 for axis in range(len(extent))])
    return level


def setup_inputs(seed: int = 0) -> dict:
    splits = jax.random.split(jax.random.key(seed), 7)
    return {
        "q_raw": draw_q_raw(jax.random.fold_in(splits[6], 71), 0),
        "k_raw": draw_k_raw(jax.random.fold_in(splits[6], 71), 0),
        "v_raw": draw_v_raw(jax.random.fold_in(splits[6], 71), 0),
        "block_scales": jnp.clip(jnp.exp(math.log(4.0) - 2.7725887 * jax.random.uniform(splits[3], (3, SEQ // BLK, H), jnp.float32) ** level_of(splits[3], (3, SEQ // BLK, H), ((1, 128), (2, 4)), -0.2, 0.2)), 0.25, 4.0),
        "segment_ids": draw_segment_ids(jax.random.fold_in(splits[6], 71), 0),
        "norm_gain": jnp.clip(1.0 + 0.1 * jax.random.normal(splits[5], (H * HD,), jnp.float32), 0.5, 1.5),
    }


epsilon = 1e-06

def seg_add(left, right):
    left_flag, left_value = left
    right_flag, right_value = right
    return (jnp.maximum(left_flag, right_flag), right_value + (1.0 - right_flag) * left_value)

def reference(q_raw, k_raw, v_raw, block_scales, segment_ids, norm_gain):
    seg_total = CAP * N_SEQ + 1
    half_len = TOK_DEV // 2
    block_count = SEQ // half_len
    score_scale = 1.0 / HD ** 0.5
    positions = jnp.arange(SEQ, dtype=jnp.int32)
    unit_weights = jnp.ones((SEQ, 1), jnp.float32)
    seg_counts = jax.ops.segment_sum(jnp.ones((SEQ,), jnp.float32), segment_ids, num_segments=seg_total)
    seg_size = jnp.maximum(seg_counts, 1.0)
    seg_bias = jnp.log(seg_size)
    start_flags = jnp.concatenate([jnp.ones((1, 1), jnp.float32), (segment_ids[1:] != segment_ids[:-1]).astype(jnp.float32)[:, None]], axis=0)
    run_count = lax.associative_scan(seg_add, (start_flags, unit_weights))[1][:, 0]
    block_index = positions // half_len
    edge_index = jnp.maximum((block_index - 1) * half_len - 1, 0).astype(jnp.int32)
    run_live = (block_index >= 1) & (segment_ids[edge_index] == segment_ids)
    run_total = jnp.where(run_live, run_count[edge_index], 0.0)
    run_size = jnp.maximum(run_total, 1.0)
    seg_order = jnp.arange(seg_total, dtype=jnp.int32)
    pad_ids = jnp.concatenate([jnp.full((half_len,), -1, jnp.int32), segment_ids])

    def one_head(head_index):

        def dequantize(raw, which):
            piece = lax.dynamic_slice_in_dim(raw, head_index * HD, HD, 1).astype(jnp.float32)
            factor = jnp.repeat(block_scales[which, :, head_index], BLK)[:, None]
            return (piece * factor).astype(jnp.bfloat16)
        head_query = dequantize(q_raw, 0)
        head_key = dequantize(k_raw, 1)
        head_value = dequantize(v_raw, 2)
        key_float = head_key.astype(jnp.float32)
        value_float = head_value.astype(jnp.float32)
        land_key = (jax.ops.segment_sum(key_float, segment_ids, num_segments=seg_total) / seg_size[:, None]).astype(jnp.bfloat16)
        land_value = (jax.ops.segment_sum(value_float, segment_ids, num_segments=seg_total) / seg_size[:, None]).astype(jnp.bfloat16)
        run_key = lax.associative_scan(seg_add, (start_flags, key_float))[1]
        run_value = lax.associative_scan(seg_add, (start_flags, value_float))[1]
        run_key = jnp.where(run_live[:, None], run_key[edge_index], 0.0) / run_size[:, None]
        run_value = jnp.where(run_live[:, None], run_value[edge_index], 0.0) / run_size[:, None]
        pad_key = jnp.concatenate([jnp.zeros((half_len, HD), jnp.bfloat16), head_key], axis=0)
        pad_value = jnp.concatenate([jnp.zeros((half_len, HD), jnp.bfloat16), head_value], axis=0)

        def one_block(block):
            row_start = (block * half_len).astype(jnp.int32)
            query_rows = lax.dynamic_slice_in_dim(head_query, row_start, half_len, 0)
            query_ids = lax.dynamic_slice_in_dim(segment_ids, row_start, half_len, 0)
            key_rows = lax.dynamic_slice_in_dim(pad_key, row_start, 2 * half_len, 0)
            value_rows = lax.dynamic_slice_in_dim(pad_value, row_start, 2 * half_len, 0)
            key_ids = lax.dynamic_slice_in_dim(pad_ids, row_start, 2 * half_len, 0)
            query_pos = row_start + jnp.arange(half_len, dtype=jnp.int32)
            key_pos = row_start - half_len + jnp.arange(2 * half_len, dtype=jnp.int32)
            win_mask = (key_ids[None, :] == query_ids[:, None]) & (key_pos[None, :] <= query_pos[:, None])
            win_score = jnp.dot(query_rows, key_rows.T, preferred_element_type=jnp.float32) * score_scale
            win_score = jnp.where(win_mask, win_score, -jnp.inf)
            land_score = jnp.dot(query_rows, land_key.T, preferred_element_type=jnp.float32) * score_scale + seg_bias[None, :]
            land_score = jnp.where(seg_order[None, :] < query_ids[:, None], land_score, -jnp.inf)
            live_rows = lax.dynamic_slice_in_dim(run_live, row_start, half_len, 0)
            rows_key = lax.dynamic_slice_in_dim(run_key, row_start, half_len, 0)
            rows_value = lax.dynamic_slice_in_dim(run_value, row_start, half_len, 0)
            rows_size = lax.dynamic_slice_in_dim(run_size, row_start, half_len, 0)
            run_score = lax.optimization_barrier(jnp.sum(query_rows.astype(jnp.float32) * rows_key, axis=1)) * score_scale + jnp.log(rows_size)
            run_score = jnp.where(live_rows, run_score, -jnp.inf)
            row_max = jnp.maximum(jnp.maximum(lax.optimization_barrier(jnp.max(win_score, axis=1)), lax.optimization_barrier(jnp.max(land_score, axis=1))), run_score)
            win_weight = jnp.exp(win_score - row_max[:, None])
            land_weight = jnp.exp(land_score - row_max[:, None])
            run_weight = jnp.exp(run_score - row_max)
            row_total = lax.optimization_barrier(jnp.sum(win_weight, axis=1)) + lax.optimization_barrier(jnp.sum(land_weight, axis=1)) + run_weight
            weighted = jnp.dot(win_weight.astype(jnp.bfloat16), value_rows, preferred_element_type=jnp.float32)
            weighted = weighted + jnp.dot(land_weight.astype(jnp.bfloat16), land_value, preferred_element_type=jnp.float32)
            weighted = weighted + run_weight[:, None] * rows_value
            return weighted / row_total[:, None]
        blocks = lax.map(one_block, jnp.arange(block_count, dtype=jnp.int32))
        return blocks.reshape(SEQ, HD)
    attention = lax.map(one_head, jnp.arange(H, dtype=jnp.int32))
    mean_square = lax.optimization_barrier(jnp.sum(attention * attention, axis=(0, 2))) / (H * HD)
    scaled = attention * lax.rsqrt(mean_square + epsilon)[None, :, None]
    return (jnp.transpose(scaled, (1, 0, 2)).reshape(SEQ, H * HD) * norm_gain[None, :]).astype(jnp.bfloat16)
```

```python
import functools
import jax
import jax.numpy as jnp
from jax import lax
from jax.experimental import pallas as pl
from jax.experimental.pallas import tpu as pltpu
from jax.sharding import PartitionSpec as P

HEADS = 32
HD = 128
CAP = 4
BLK = 128
SCALE = 1.0 / HD**0.5
LOG2E = 1.4426950408889634
EXP_SCALE = SCALE * LOG2E
NEG = -1e30
EPS = 1e-6
NX, NZ, NC = 4, 16, 2
MESH = pl.DeviceIdType.MESH
F32 = jnp.float32
BF16 = jnp.bfloat16
NT = (((1,), (1,)), ((), ()))


def dot(a, b):
    return jnp.dot(a, b, preferred_element_type=F32)


def dot_nt(a, b):
    return lax.dot_general(a, b, NT, preferred_element_type=F32)


def iota(shape, dim):
    return lax.broadcasted_iota(jnp.int32, shape, dim)


def kernel(
    dims,
    q_hbm, k_hbm, v_hbm, scales, seg_ref, gain_ref,
    out_ref,
    raw_q, raw_k, raw_v, qd, kx, vx,
    packet, pbuf, lmk, lkf, lvf, tab, kaux, qaux, ekh, ekl, evv, lbias,
    maskb, acc, mrow, squares, ssbuf,
    in_sem, halo_s, halo_r, ps, pr, zs, zr, xs, xr, ds, dr, ys, yr,
):
    nx, nz, ny = dims
    pairs = nz // 2
    ndev = nx * nz * NC
    tok, width = out_ref.shape
    half = tok // 2
    heads = width // HD
    d = lax.axis_index("seq")
    y = lax.axis_index("head")
    core = lax.rem(d, 2)
    zpos = lax.rem(lax.div(d, 2), nz)
    xpos = lax.div(d, 2 * nz)
    pair = lax.div(zpos, 2)
    group = lax.div(d, 4)
    ngroups = ndev // 4
    member = lax.rem(d, 4)
    sgn = 1 - 2 * core
    partner = d + sgn

    def at(x, z, c):
        return (x * nz + z) * 2 + c

    loads = [
        pltpu.make_async_copy(src, dst, in_sem.at[n])
        for n, (src, dst) in enumerate(((k_hbm, raw_k), (v_hbm, raw_v), (q_hbm, raw_q)))
    ]
    for load in loads:
        load.start()

    znext = lax.rem(zpos + 2 * sgn + nz, nz)
    zprev = lax.rem(zpos - 2 * sgn + nz, nz)
    peers = [group * 4 + lax.rem(member + n, 4) for n in (1, 2, 3)]
    nextg = [lax.rem(group + 1, ngroups) * 4 + n for n in range(4)]
    prevg = [lax.rem(group + ngroups - 1, ngroups) * 4 + n for n in range(4)]
    xpeers = [at(lax.rem(xpos + n, nx), zpos, core) for n in range(1, nx)]
    zpeers = [at(xpos, znext, core), at(xpos, zprev, core)]
    ypeers = [lax.rem(y + n, ny) for n in range(1, ny)]
    barrier = pltpu.get_barrier_semaphore()
    greeted = peers + nextg + prevg + xpeers + zpeers
    for peer in greeted:
        pl.semaphore_signal(barrier, inc=1, device_id={"seq": peer}, device_id_type=MESH)
    for peer in ypeers:
        pl.semaphore_signal(barrier, inc=1, device_id={"head": peer}, device_id_type=MESH)

    seg = seg_ref[...]
    first = jnp.min(seg, axis=1, keepdims=True)
    last = jnp.max(seg, axis=1, keepdims=True)
    end = last - first
    local = seg - first
    endf = end.astype(F32)
    row = iota((16, tok), 0)
    pos = iota((16, tok), 1)
    slot = lax.rem(row, 4)
    wide = jnp.broadcast_to(local, (16, tok))
    is_slot = (row < 8) & (wide == slot) & (slot < end)
    is_tail = (row >= 8) & (wide == end) & (lax.rem(row, 2) == lax.div(pos, half))
    pick32 = jnp.where(is_slot | is_tail, 1.0, 0.0)
    pick = pick32.astype(BF16)
    counts = jnp.sum(pick32, axis=1, keepdims=True)
    r16 = iota((16, HD), 0)
    l16 = iota((16, HD), 1)
    want = jnp.where(r16 < 4, r16, jnp.where((r16 >= 8) & (r16 < 10), r16 - 4, -1))
    count_row = jnp.sum(jnp.where(l16 == want, counts, 0.0), axis=0, keepdims=True)
    lane = iota((1, HD), 1)
    count_row = jnp.where(lane == 6, endf, count_row)
    count_wide = jnp.concatenate([count_row] + [jnp.zeros((1, HD), F32)] * (heads - 1), axis=1)

    def dequantize(src, which, dst, base):
        def block(b, _):
            for h in range(heads):
                factor = scales[which, b, h]
                rows = pl.ds(pl.multiple_of(b * BLK, BLK), BLK)
                piece = src[rows, h * HD : (h + 1) * HD].astype(F32) * factor
                dst[pl.ds(pl.multiple_of(base + b * BLK, BLK), BLK), h * HD : (h + 1) * HD] = (
                    piece.astype(BF16)
                )
            return 0

        lax.fori_loop(0, tok // BLK, block, 0)

    loads[0].wait()
    dequantize(raw_k, 1, kx, half)
    key_sums = dot(pick, kx[half:, :])
    loads[1].wait()
    dequantize(raw_v, 2, vx, half)
    value_sums = dot(pick, vx[half:, :])
    r8 = iota((8, width), 0)
    packet[0] = jnp.where(r8 < 4, key_sums[0:8], value_sums[0:8])
    packet[1] = jnp.where(
        r8 < 2, key_sums[8:16], jnp.where(r8 == 4, count_wide, value_sums[8:16])
    )

    pl.semaphore_wait(barrier, len(greeted) + len(ypeers))

    sends = []
    for n, peer in enumerate(peers):
        sends.append(
            pltpu.make_async_remote_copy(
                src_ref=packet, dst_ref=pbuf.at[1 + member], send_sem=ps.at[n],
                recv_sem=pr.at[1 + member], device_id={"seq": peer}, device_id_type=MESH,
            )
        )
    for copy in sends:
        copy.start()

    def tail_copy(n):
        return pltpu.make_async_remote_copy(
            src_ref=packet.at[1], dst_ref=pbuf.at[0, 1], send_sem=ps.at[3 + n],
            recv_sem=pr.at[0], device_id={"seq": nextg[n]}, device_id_type=MESH,
        )

    sends_on = (member == 3) & (group < ngroups - 1)

    @pl.when(sends_on)
    def _():
        for n in range(4):
            tail_copy(n).start()

    follower = lax.rem(d + 1, ndev)

    def halo_copy(n, ref):
        return pltpu.make_async_remote_copy(
            src_ref=ref.at[pl.ds(tok, half)], dst_ref=ref.at[pl.ds(0, half)],
            send_sem=halo_s.at[n], recv_sem=halo_r.at[n],
            device_id={"seq": follower}, device_id_type=MESH,
        )

    @pl.when(d < ndev - 1)
    def _():
        halo_copy(0, kx).start()
        halo_copy(1, vx).start()

    @pl.when(d == 0)
    def _():
        kx[0:half, :] = jnp.zeros((half, width), BF16)
        vx[0:half, :] = jnp.zeros((half, width), BF16)

    @pl.when(group == 0)
    def _():
        pbuf[0, 1] = jnp.zeros((8, width), F32)

    for r in range(1, nx):
        @pl.when(xpos < r)
        def _():
            tab[r * pairs : (r + 1) * pairs] = jnp.zeros((pairs, 16, tab.shape[2]), BF16)

    pbuf[1 + member] = packet[...]
    for n in (1, 2, 3):
        other = lax.rem(member + n, 4)
        pltpu.make_async_remote_copy(
            src_ref=packet, dst_ref=pbuf.at[1 + other], send_sem=ps.at[0],
            recv_sem=pr.at[1 + other], device_id={"seq": peers[0]}, device_id_type=MESH,
        ).wait_recv()

    @pl.when(group > 0)
    def _():
        tail_copy(0).wait_recv()

    lead = group == 0
    r8n = iota((8, HD), 0)
    l8n = iota((8, HD), 1)
    tails = [pbuf[n, 1] for n in range(5)]

    def whole_tail(t):
        return t[0:1] + t[1:2], t[2:3] + t[3:4], t[4:5, 4:5] + t[4:5, 5:6]

    for j in range(4):
        key_tail, value_tail, tail_count = whole_tail(tails[j])
        for back in range(1, j):
            extra = whole_tail(tails[j - back])
            key_tail = key_tail + jnp.where(lead, extra[0], 0.0)
            value_tail = value_tail + jnp.where(lead, extra[1], 0.0)
            tail_count = tail_count + jnp.where(lead, extra[2], 0.0)
        total = pbuf[1 + j, 0]
        total = total + jnp.where(r8 == 0, key_tail, jnp.where(r8 == 4, value_tail, 0.0))
        crow = tails[j + 1][4:5, 0:HD]
        slot8 = lax.rem(r8n, 4)
        number = jnp.sum(jnp.where(l8n == slot8, crow, 0.0), axis=1, keepdims=True)
        rc = iota((8, 1), 0)
        number = number + jnp.where(lax.rem(rc, 4) == 0, tail_count, 0.0)
        number = jnp.maximum(number, 1.0)
        done = (lax.rem(rc, 4)).astype(F32) < crow[0:1, 6:7]
        value = total / number
        lmk[...] = value
        lkf[4 * j : 4 * j + 4, :] = lmk[0:4, :]
        lvf[4 * j : 4 * j + 4, :] = lmk[4:8, :]
        bias = jnp.where(done, jnp.log(number) * (1.0 / SCALE), NEG)
        lbias[4 * j : 4 * j + 4, :] = jnp.broadcast_to(bias, (8, HD))[0:4]

    own_bias = lbias[...]
    hi = own_bias.astype(BF16).astype(F32)
    mid = (own_bias - hi).astype(BF16).astype(F32)
    low = own_bias - hi - mid
    aux = jnp.where(l16 == 0, hi, jnp.where(l16 == 1, mid, jnp.where(l16 == 2, low, 0.0)))
    own_keys = lkf[...].astype(BF16)
    own_values = lvf[...].astype(BF16)
    tab[group, :, 0:width] = own_keys
    tab[group, :, width : 2 * width] = own_values
    tab[group, :, 2 * width :] = aux.astype(BF16)

    def chunk_copy(row_x, p, send_sem, recv_sem, target):
        g = row_x * pairs + p
        return pltpu.make_async_remote_copy(
            src_ref=tab.at[g], dst_ref=tab.at[g], send_sem=send_sem, recv_sem=recv_sem,
            device_id={"seq": target}, device_id_type=MESH,
        )

    def ring_pair(i, c_sgn):
        return lax.rem(pair - c_sgn * i + 2 * pairs, pairs)

    steps = pairs // 2

    def ring_send(i):
        return chunk_copy(xpos, ring_pair(i - 1, sgn), zs.at[i - 1], zr.at[i - 1],
                          at(xpos, znext, core))

    def ring_recv(i):
        return chunk_copy(xpos, ring_pair(i, sgn), zs.at[i - 1], zr.at[i - 1],
                          at(xpos, znext, core))

    def row_send(dx, i):
        return chunk_copy(xpos, ring_pair(i, sgn), xs.at[dx - 1, i], xr.at[dx - 1, i],
                          at(lax.rem(xpos + dx, nx), zpos, core))

    def row_recv(dx, i):
        return chunk_copy(xpos - dx, ring_pair(i, sgn), xs.at[dx - 1, i], xr.at[dx - 1, i],
                          at(lax.rem(xpos + dx, nx), zpos, core))

    def pass_on(dx, i):
        return chunk_copy(xpos - dx, ring_pair(i, sgn), ds.at[dx, i], dr.at[dx, i], partner)

    def passed(dx, i):
        return chunk_copy(xpos - dx, ring_pair(i, -sgn), ds.at[dx, i], dr.at[dx, i], partner)

    def if_core0(i, extra=None):
        conds = []
        if i == 0 or i == steps:
            conds.append(core == 0)
        if extra is not None:
            conds.append(extra)
        return functools.reduce(jnp.logical_and, conds) if conds else None

    def if_core1_partner(i, extra=None):
        conds = []
        if i == 0 or i == steps:
            conds.append(core == 1)
        if extra is not None:
            conds.append(extra)
        return functools.reduce(jnp.logical_and, conds) if conds else None

    def run_if(cond, fn):
        if cond is None:
            fn()
        else:
            pl.when(cond)(fn)

    def ring_start(i):
        run_if(if_core0(i), lambda: ring_send(i).start())

    def row_start(i):
        for dx in range(1, nx):
            run_if(if_core0(i, xpos + dx < nx), lambda: row_send(dx, i).start())

    ring_start(1)
    row_start(0)

    before = pbuf[member, 1]
    one_back = pbuf[jnp.maximum(member - 1, 0), 1]
    two_back = pbuf[jnp.maximum(member - 2, 0), 1]
    ext2 = lead & (member >= 2)
    ext3 = lead & (member == 3)

    def extra_tail(r0, c0):
        value2 = one_back[r0 : r0 + 1] + one_back[r0 + 1 : r0 + 2]
        value3 = two_back[r0 : r0 + 1] + two_back[r0 + 1 : r0 + 2]
        return jnp.where(ext2, value2, 0.0) + jnp.where(ext3, value3, 0.0)

    extra_count = jnp.where(ext2, one_back[4:5, 4:5] + one_back[4:5, 5:6], 0.0) + jnp.where(
        ext3, two_back[4:5, 4:5] + two_back[4:5, 5:6], 0.0
    )
    prev_count = before[4:5, 5:6]
    early_count = before[4:5, 4:5] + extra_count
    late_count = early_count + prev_count
    early_size = jnp.maximum(early_count, 1.0)
    late_size = jnp.maximum(late_count, 1.0)
    early_key = before[0:1] + extra_tail(0, 0)
    late_key = (early_key + before[1:2]) / late_size
    early_key = early_key / early_size
    early_value = before[2:3] + extra_tail(2, 0)
    late_value = (early_value + before[3:4]) / late_size
    early_value = early_value / early_size
    rw = iota((16, width), 0)
    run_keys = jnp.where(rw == 0, early_key, jnp.where(rw == 1, late_key, 0.0))
    run_hi = run_keys.astype(BF16)
    run_lo = (run_keys - run_hi.astype(F32)).astype(BF16)
    run_values = jnp.where(rw == 0, early_value, jnp.where(rw == 1, late_value, 0.0))
    ekh[0:16, :] = own_keys
    ekh[16:32, :] = run_hi
    ekh[32:, :] = jnp.zeros((HD - 32, width), BF16)
    ekl[0:16, :] = jnp.zeros((16, width), BF16)
    ekl[16:32, :] = run_lo
    ekl[32:, :] = jnp.zeros((HD - 32, width), BF16)
    evv[0:16, :] = own_values
    evv[16:32, :] = run_values.astype(BF16)
    evv[32:, :] = jnp.zeros((HD - 32, width), BF16)

    columns = jnp.broadcast_to(local.astype(F32), (HD, tok)).T
    own_row = jnp.sum(jnp.where(l16 == r16, own_bias, 0.0), axis=0, keepdims=True)
    early_bias = jnp.where(early_count > 0.5, jnp.log(early_size) * (1.0 / SCALE), NEG)
    late_bias = jnp.where(late_count > 0.5, jnp.log(late_size) * (1.0 / SCALE), NEG)
    key_row = jnp.concatenate(
        [jnp.where(iota((1, half), 1).astype(F32) >= half - prev_count, 0.0, -1.0),
         local.astype(F32)], axis=1,
    )
    el = iota((half, HD), 1)
    owner = lax.div(el, 4)
    for b in range(2):
        mine = columns[b * half : (b + 1) * half]
        wide_mine = jnp.concatenate([mine] * (tok // HD), axis=1)
        keys = key_row[:, b * half : b * half + tok]
        i_pos = iota((half, tok), 0) + half
        j_pos = iota((half, tok), 1)
        ok = (wide_mine == keys) & (j_pos <= i_pos)
        maskb[b, :, 0:tok] = jnp.where(ok, 0.0, NEG)
        visible = (el < 16) & (
            (owner < member) | ((owner == member) & (lax.rem(el, 4).astype(F32) < mine))
        )
        run_bias = early_bias if b == 0 else late_bias
        run_ok = (el == 16 + b) & (mine == 0.0)
        maskb[b, :, tok:] = jnp.where(visible, own_row, jnp.where(run_ok, run_bias, NEG))
    qaux[...] = jnp.where(iota((half, HD), 1) < 3, 1.0, 0.0).astype(BF16)
    loads[2].wait()
    dequantize(raw_q, 0, qd, 0)

    ones_tok = jnp.ones((tok, HD), BF16)
    ones_ext = jnp.ones((HD, HD), BF16)

    def window(h, b):
        lanes = pl.ds(pl.multiple_of(h * HD, HD), HD)
        q = qd[b * half : (b + 1) * half, lanes]
        keys = kx[b * half : b * half + tok, lanes]
        ext = jnp.concatenate([ekh[:, lanes], ekl[:, lanes]], axis=1)
        s = jnp.concatenate(
            [dot_nt(q, keys), dot_nt(jnp.concatenate([q, q], axis=1), ext)], axis=1
        ) + maskb[b]
        m = jnp.max(s, axis=1, keepdims=True)
        p = jnp.exp2((s - m) * EXP_SCALE).astype(BF16)
        v = jnp.concatenate([vx[b * half : b * half + tok, lanes], ones_tok], axis=1)
        ev = jnp.concatenate([evv[:, lanes], ones_ext], axis=1)
        acc[h, b * half : (b + 1) * half, :] = dot(p[:, :tok], v) + dot(p[:, tok:], ev)
        mrow[h, b * half : (b + 1) * half, :] = jnp.broadcast_to(m, (half, HD))

    def windows(lo, hi, b):
        def body(h, _):
            window(h, b)
            return 0

        lax.fori_loop(lo, hi, body, 0)

    share = heads // steps

    def landed(i):
        def go():
            ring_recv(i).wait_recv()
            if i < steps:
                ring_start(i + 1)

        run_if(if_core0(i), go)
        row_start(i)
        run_if(if_core0(i), lambda: pass_on(0, i).start())

    for i in range(1, steps + 1):
        landed(i)
        windows((i - 1) * share, i * share, 1)

    def rows_landed(i):
        for dx in range(1, nx):
            def go():
                row_recv(dx, i).wait_recv()
                pass_on(dx, i).start()

            run_if(if_core0(i, xpos >= dx), go)

    for i in range(0, steps - 1):
        rows_landed(i)

    @pl.when(d > 0)
    def _():
        halo_copy(0, kx).wait_recv()
        halo_copy(1, vx).wait_recv()

    windows(0, heads // 2, 0)
    for i in range(steps - 1, steps + 1):
        rows_landed(i)
    windows(heads // 2, heads, 0)
    for dx in range(nx):
        for i in range(0 if dx else 1, steps + 1):
            run_if(
                if_core1_partner(i, (xpos >= dx) if dx else None),
                lambda: passed(dx, i).wait_recv(),
            )

    nkeys = ngroups * 16
    flat_aux = tab[:, :, 2 * width :].reshape(nkeys, HD)
    key_group = lax.div(iota((nkeys, HD), 0), 16)
    off = jnp.where(iota((nkeys, HD), 1) == 0, NEG, 0.0)
    kaux[...] = jnp.where(key_group < group, flat_aux.astype(F32), off).astype(BF16)
    squares[...] = jnp.zeros(squares.shape, F32)
    ones_key = jnp.ones((nkeys, HD), BF16)

    def landmarks(h, _):
        lanes = pl.ds(pl.multiple_of(h * HD, HD), HD)
        vlanes = pl.ds(pl.multiple_of(width + h * HD, HD), HD)
        keys = jnp.concatenate([tab[:, :, lanes].reshape(nkeys, HD), kaux[...]], axis=1)
        values = jnp.concatenate([tab[:, :, vlanes].reshape(nkeys, HD), ones_key], axis=1)
        for b in range(2):
            rows = slice(b * half, (b + 1) * half)
            q = jnp.concatenate([qd[rows, lanes], qaux[...]], axis=1)
            s = dot_nt(q, keys)
            old = mrow[h, rows, :]
            m = jnp.maximum(old, jnp.max(s, axis=1, keepdims=True))
            fade = jnp.exp2((old - m) * EXP_SCALE)
            p = jnp.exp2((s - jnp.concatenate([m] * (nkeys // HD), axis=1)) * EXP_SCALE)
            o = dot(p.astype(BF16), values)
            prior = acc[h, rows, :]
            top = prior[:, :HD] * fade + o[:, :HD]
            bottom = prior[:, HD:] * fade + o[:, HD:]
            a = top / bottom
            acc[h, rows, 0:HD] = a
            squares[rows, :] += a * a
        return 0

    lax.fori_loop(0, heads, landmarks, 0)

    ssbuf[0] = jnp.broadcast_to(jnp.sum(squares[...].T, axis=0, keepdims=True), (8, tok))

    def square_copy(n):
        return pltpu.make_async_remote_copy(
            src_ref=ssbuf.at[0], dst_ref=ssbuf.at[n + 1], send_sem=ys.at[n],
            recv_sem=yr.at[n], device_id={"head": ypeers[n]}, device_id_type=MESH,
        )

    for n in range(ny - 1):
        square_copy(n).start()
    for n in range(ny - 1):
        square_copy(n).wait_recv()
    total = ssbuf[0, 0:1]
    for n in range(1, ny):
        total = total + ssbuf[n, 0:1]
    norm = lax.rsqrt(total / (heads * ny * HD) + EPS)
    norm = jnp.broadcast_to(norm, (HD, tok)).T
    for h in range(heads):
        out_ref[:, h * HD : (h + 1) * HD] = (
            acc[h, :, 0:HD] * norm * gain_ref[:, h * HD : (h + 1) * HD]
        ).astype(BF16)

    for copy in sends:
        copy.wait_send()

    @pl.when(sends_on)
    def _():
        for n in range(4):
            tail_copy(n).wait_send()

    @pl.when(d < ndev - 1)
    def _():
        halo_copy(0, kx).wait_send()
        halo_copy(1, vx).wait_send()

    for i in range(1, steps + 1):
        run_if(if_core0(i), lambda: ring_send(i).wait_send())
    for i in range(0, steps + 1):
        for dx in range(1, nx):
            run_if(if_core0(i, xpos + dx < nx), lambda: row_send(dx, i).wait_send())
        for dx in range(nx):
            if dx or i:
                run_if(
                    if_core0(i, (xpos >= dx) if dx else None),
                    lambda: pass_on(dx, i).wait_send(),
                )
    for n in range(ny - 1):
        square_copy(n).wait_send()


def solution(mesh, nx=NX, nz=NZ):
    ny = mesh.shape["head"]

    def on_device(q_raw, k_raw, v_raw, block_scales, segment_ids, norm_gain):
        tok, width = q_raw.shape
        heads = width // HD
        half = tok // 2
        groups = nx * nz // 2
        steps = nz // 4
        dma = pltpu.SemaphoreType.DMA
        hbm = pl.BlockSpec(memory_space=pl.ANY)
        vmem = pl.BlockSpec(memory_space=pltpu.VMEM)
        smem = pl.BlockSpec(memory_space=pltpu.SMEM)
        return pl.pallas_call(
            functools.partial(kernel, (nx, nz, ny)),
            out_shape=jax.ShapeDtypeStruct((tok, width), BF16),
            in_specs=[hbm, hbm, hbm, smem, vmem, vmem],
            out_specs=vmem,
            scratch_shapes=[
                pltpu.VMEM((tok, width), BF16),
                pltpu.VMEM((tok, width), BF16),
                pltpu.VMEM((tok, width), BF16),
                pltpu.VMEM((tok, width), BF16),
                pltpu.VMEM((tok + half, width), BF16),
                pltpu.VMEM((tok + half, width), BF16),
                pltpu.VMEM((2, 8, width), F32),
                pltpu.VMEM((5, 2, 8, width), F32),
                pltpu.VMEM((8, width), F32),
                pltpu.VMEM((16, width), F32),
                pltpu.VMEM((16, width), F32),
                pltpu.VMEM((groups, 16, 2 * width + HD), BF16),
                pltpu.VMEM((groups * 16, HD), BF16),
                pltpu.VMEM((half, HD), BF16),
                pltpu.VMEM((HD, width), BF16),
                pltpu.VMEM((HD, width), BF16),
                pltpu.VMEM((HD, width), BF16),
                pltpu.VMEM((16, HD), F32),
                pltpu.VMEM((2, half, tok + HD), F32),
                pltpu.VMEM((heads, tok, 2 * HD), F32),
                pltpu.VMEM((heads, tok, HD), F32),
                pltpu.VMEM((tok, HD), F32),
                pltpu.VMEM((ny, 8, tok), F32),
                dma((3,)), dma((2,)), dma((2,)), dma((7,)), dma((5,)),
                dma((steps,)), dma((steps,)),
                dma((nx - 1, steps + 1)), dma((nx - 1, steps + 1)),
                dma((nx, steps + 1)), dma((nx, steps + 1)),
                dma((max(ny - 1, 1),)), dma((max(ny - 1, 1),)),
            ],
            compiler_params=pltpu.CompilerParams(
                collective_id=0, has_side_effects=True, vmem_limit_bytes=60000000
            ),
            name="attention",
        )(
            q_raw, k_raw, v_raw, block_scales,
            segment_ids.reshape(1, tok), norm_gain.reshape(1, width),
        )

    in_specs = (
        P("seq", "head"),
        P("seq", "head"),
        P("seq", "head"),
        P(None, "seq", "head"),
        P("seq"),
        P("head"),
    )
    return jax.shard_map(
        on_device, mesh=mesh, in_specs=in_specs, out_specs=P("seq", "head"), check_vma=False
    )
```

```python
import functools
import jax
import jax.numpy as jnp
from jax import lax
from jax.experimental import pallas as pl
from jax.experimental.pallas import tpu as pltpu
from jax.sharding import PartitionSpec as P

HEADS = 32
HD = 128
CAP = 4
BLK = 128
SCALE = 1.0 / HD**0.5
LOG2E = 1.4426950408889634
EXP_SCALE = SCALE * LOG2E
NEG = -1e30
EPS = 1e-6
NX, NZ, NC = 4, 16, 2
MESH = pl.DeviceIdType.MESH
F32 = jnp.float32
BF16 = jnp.bfloat16
NT = (((1,), (1,)), ((), ()))


def dot(a, b):
    return jnp.dot(a, b, preferred_element_type=F32)


def dot_nt(a, b):
    return lax.dot_general(a, b, NT, preferred_element_type=F32)


def iota(shape, dim):
    return lax.broadcasted_iota(jnp.int32, shape, dim)


def kernel(
    dims,
    q_hbm, k_hbm, v_hbm, scales, seg_ref,
    out_ref,
    raw_q, raw_k, raw_v, qd, kx, vx,
    packet, pbuf, lmk, lkf, lvf, tab, kaux, qaux, ekh, ekl, evv, lbias,
    maskb, acc, mrow, squares, ssbuf,
    in_sem, halo_s, halo_r, ps, pr, zs, zr, xs, xr, ds, dr, ys, yr,
):
    nx, nz, ny = dims
    pairs = nz // 2
    ndev = nx * nz * NC
    tok, width = out_ref.shape
    half = tok // 2
    heads = width // HD
    d = lax.axis_index("seq")
    y = lax.axis_index("head")
    core = lax.rem(d, 2)
    zpos = lax.rem(lax.div(d, 2), nz)
    xpos = lax.div(d, 2 * nz)
    pair = lax.div(zpos, 2)
    group = lax.div(d, 4)
    ngroups = ndev // 4
    member = lax.rem(d, 4)
    sgn = 1 - 2 * core
    partner = d + sgn

    def at(x, z, c):
        return (x * nz + z) * 2 + c

    loads = [
        pltpu.make_async_copy(src, dst, in_sem.at[n])
        for n, (src, dst) in enumerate(((k_hbm, raw_k), (v_hbm, raw_v), (q_hbm, raw_q)))
    ]
    for load in loads:
        load.start()

    znext = lax.rem(zpos + 2 * sgn + nz, nz)
    zprev = lax.rem(zpos - 2 * sgn + nz, nz)
    peers = [group * 4 + lax.rem(member + n, 4) for n in (1, 2, 3)]
    nextg = [lax.rem(group + 1, ngroups) * 4 + n for n in range(4)]
    prevg = [lax.rem(group + ngroups - 1, ngroups) * 4 + n for n in range(4)]
    xpeers = [at(lax.rem(xpos + n, nx), zpos, core) for n in range(1, nx)]
    zpeers = [at(xpos, znext, core), at(xpos, zprev, core)]
    ypeers = [lax.rem(y + n, ny) for n in range(1, ny)]
    barrier = pltpu.get_barrier_semaphore()
    greeted = peers + nextg + prevg + xpeers + zpeers
    for peer in greeted:
        pl.semaphore_signal(barrier, inc=1, device_id={"seq": peer}, device_id_type=MESH)
    for peer in ypeers:
        pl.semaphore_signal(barrier, inc=1, device_id={"head": peer}, device_id_type=MESH)

    seg = seg_ref[...]
    first = jnp.min(seg, axis=1, keepdims=True)
    last = jnp.max(seg, axis=1, keepdims=True)
    end = last - first
    local = seg - first
    endf = end.astype(F32)
    row = iota((16, tok), 0)
    pos = iota((16, tok), 1)
    slot = lax.rem(row, 4)
    wide = jnp.broadcast_to(local, (16, tok))
    is_slot = (row < 8) & (wide == slot) & (slot < end)
    is_tail = (row >= 8) & (wide == end) & (lax.rem(row, 2) == lax.div(pos, half))
    pick32 = jnp.where(is_slot | is_tail, 1.0, 0.0)
    pick = pick32.astype(BF16)
    counts = jnp.sum(pick32, axis=1, keepdims=True)
    r16 = iota((16, HD), 0)
    l16 = iota((16, HD), 1)
    want = jnp.where(r16 < 4, r16, jnp.where((r16 >= 8) & (r16 < 10), r16 - 4, -1))
    count_row = jnp.sum(jnp.where(l16 == want, counts, 0.0), axis=0, keepdims=True)
    lane = iota((1, HD), 1)
    count_row = jnp.where(lane == 6, endf, count_row)
    count_wide = jnp.concatenate([count_row] + [jnp.zeros((1, HD), F32)] * (heads - 1), axis=1)

    def dequantize(src, which, dst, base):
        def block(b, _):
            for h in range(heads):
                factor = scales[which, b, h]
                rows = pl.ds(pl.multiple_of(b * BLK, BLK), BLK)
                piece = src[rows, h * HD : (h + 1) * HD].astype(F32) * factor
                dst[pl.ds(pl.multiple_of(base + b * BLK, BLK), BLK), h * HD : (h + 1) * HD] = (
                    piece.astype(BF16)
                )
            return 0

        lax.fori_loop(0, tok // BLK, block, 0)

    loads[0].wait()
    dequantize(raw_k, 1, kx, half)
    key_sums = dot(pick, kx[half:, :])
    loads[1].wait()
    dequantize(raw_v, 2, vx, half)
    value_sums = dot(pick, vx[half:, :])
    r8 = iota((8, width), 0)
    packet[0] = jnp.where(r8 < 4, key_sums[0:8], value_sums[0:8])
    packet[1] = jnp.where(
        r8 < 2, key_sums[8:16], jnp.where(r8 == 4, count_wide, value_sums[8:16])
    )

    pl.semaphore_wait(barrier, len(greeted) + len(ypeers))

    sends = []
    for n, peer in enumerate(peers):
        sends.append(
            pltpu.make_async_remote_copy(
                src_ref=packet, dst_ref=pbuf.at[1 + member], send_sem=ps.at[n],
                recv_sem=pr.at[1 + member], device_id={"seq": peer}, device_id_type=MESH,
            )
        )
    for copy in sends:
        copy.start()

    def tail_copy(n):
        return pltpu.make_async_remote_copy(
            src_ref=packet.at[1], dst_ref=pbuf.at[0, 1], send_sem=ps.at[3 + n],
            recv_sem=pr.at[0], device_id={"seq": nextg[n]}, device_id_type=MESH,
        )

    sends_on = (member == 3) & (group < ngroups - 1)

    @pl.when(sends_on)
    def _():
        for n in range(4):
            tail_copy(n).start()

    follower = lax.rem(d + 1, ndev)

    def halo_copy(n, ref):
        return pltpu.make_async_remote_copy(
            src_ref=ref.at[pl.ds(tok, half)], dst_ref=ref.at[pl.ds(0, half)],
            send_sem=halo_s.at[n], recv_sem=halo_r.at[n],
            device_id={"seq": follower}, device_id_type=MESH,
        )

    @pl.when(d < ndev - 1)
    def _():
        halo_copy(0, kx).start()
        halo_copy(1, vx).start()

    @pl.when(d == 0)
    def _():
        kx[0:half, :] = jnp.zeros((half, width), BF16)
        vx[0:half, :] = jnp.zeros((half, width), BF16)

    @pl.when(group == 0)
    def _():
        pbuf[0, 1] = jnp.zeros((8, width), F32)

    for r in range(1, nx):
        @pl.when(xpos < r)
        def _():
            tab[r * pairs : (r + 1) * pairs] = jnp.zeros((pairs, 16, tab.shape[2]), BF16)

    columns = jnp.broadcast_to(local.astype(F32), (HD, tok)).T
    own_ids = local.astype(F32)
    for b in range(2):
        mine = columns[b * half : (b + 1) * half]
        width_b = half * (b + 1)
        wide_mine = jnp.concatenate([mine] * (width_b // HD), axis=1)
        i_pos = iota((half, width_b), 0) + b * half
        ok = (wide_mine == own_ids[:, :width_b]) & (iota((half, width_b), 1) <= i_pos)
        start = half * (1 - b)
        maskb[b, :, start:tok] = jnp.where(ok, 0.0, NEG)
    qaux[...] = jnp.where(iota((half, HD), 1) < 3, 1.0, 0.0).astype(BF16)
    loads[2].wait()
    dequantize(raw_q, 0, qd, 0)

    pbuf[1 + member] = packet[...]
    for n in (1, 2, 3):
        other = lax.rem(member + n, 4)
        pltpu.make_async_remote_copy(
            src_ref=packet, dst_ref=pbuf.at[1 + other], send_sem=ps.at[0],
            recv_sem=pr.at[1 + other], device_id={"seq": peers[0]}, device_id_type=MESH,
        ).wait_recv()

    @pl.when(group > 0)
    def _():
        tail_copy(0).wait_recv()

    lead = group == 0
    r8n = iota((8, HD), 0)
    l8n = iota((8, HD), 1)
    tails = [pbuf[n, 1] for n in range(5)]

    def whole_tail(t):
        return t[0:1] + t[1:2], t[2:3] + t[3:4], t[4:5, 4:5] + t[4:5, 5:6]

    for j in range(4):
        key_tail, value_tail, tail_count = whole_tail(tails[j])
        for back in range(1, j):
            extra = whole_tail(tails[j - back])
            key_tail = key_tail + jnp.where(lead, extra[0], 0.0)
            value_tail = value_tail + jnp.where(lead, extra[1], 0.0)
            tail_count = tail_count + jnp.where(lead, extra[2], 0.0)
        total = pbuf[1 + j, 0]
        total = total + jnp.where(r8 == 0, key_tail, jnp.where(r8 == 4, value_tail, 0.0))
        crow = tails[j + 1][4:5, 0:HD]
        slot8 = lax.rem(r8n, 4)
        number = jnp.sum(jnp.where(l8n == slot8, crow, 0.0), axis=1, keepdims=True)
        rc = iota((8, 1), 0)
        number = number + jnp.where(lax.rem(rc, 4) == 0, tail_count, 0.0)
        number = jnp.maximum(number, 1.0)
        done = (lax.rem(rc, 4)).astype(F32) < crow[0:1, 6:7]
        value = total / number
        lmk[...] = value
        lkf[4 * j : 4 * j + 4, :] = lmk[0:4, :]
        lvf[4 * j : 4 * j + 4, :] = lmk[4:8, :]
        bias = jnp.where(done, jnp.log(number) * (1.0 / SCALE), NEG)
        lbias[4 * j : 4 * j + 4, :] = jnp.broadcast_to(bias, (8, HD))[0:4]

    own_bias = lbias[...]
    hi = own_bias.astype(BF16).astype(F32)
    mid = (own_bias - hi).astype(BF16).astype(F32)
    low = own_bias - hi - mid
    aux = jnp.where(l16 == 0, hi, jnp.where(l16 == 1, mid, jnp.where(l16 == 2, low, 0.0)))
    own_keys = lkf[...].astype(BF16)
    own_values = lvf[...].astype(BF16)
    tab[group, :, 0:width] = own_keys
    tab[group, :, width : 2 * width] = own_values
    tab[group, :, 2 * width :] = aux.astype(BF16)

    def chunk_copy(row_x, p, send_sem, recv_sem, target):
        g = row_x * pairs + p
        return pltpu.make_async_remote_copy(
            src_ref=tab.at[g], dst_ref=tab.at[g], send_sem=send_sem, recv_sem=recv_sem,
            device_id={"seq": target}, device_id_type=MESH,
        )

    def ring_pair(i, c_sgn):
        return lax.rem(pair - c_sgn * i + 2 * pairs, pairs)

    steps = pairs // 2

    def ring_send(i):
        return chunk_copy(xpos, ring_pair(i - 1, sgn), zs.at[i - 1], zr.at[i - 1],
                          at(xpos, znext, core))

    def ring_recv(i):
        return chunk_copy(xpos, ring_pair(i, sgn), zs.at[i - 1], zr.at[i - 1],
                          at(xpos, znext, core))

    def row_send(dx, i):
        return chunk_copy(xpos, ring_pair(i, sgn), xs.at[dx - 1, i], xr.at[dx - 1, i],
                          at(lax.rem(xpos + dx, nx), zpos, core))

    def row_recv(dx, i):
        return chunk_copy(xpos - dx, ring_pair(i, sgn), xs.at[dx - 1, i], xr.at[dx - 1, i],
                          at(lax.rem(xpos + dx, nx), zpos, core))

    def pass_on(dx, i):
        return chunk_copy(xpos - dx, ring_pair(i, sgn), ds.at[dx, i], dr.at[dx, i], partner)

    def passed(dx, i):
        return chunk_copy(xpos - dx, ring_pair(i, -sgn), ds.at[dx, i], dr.at[dx, i], partner)

    def here(i, extra=None):
        conds = []
        if i == 0 or i == steps:
            conds.append(core == (0 if i == 0 else 1))
        if extra is not None:
            conds.append(extra)
        return functools.reduce(jnp.logical_and, conds) if conds else None

    def there(i, extra=None):
        conds = []
        if i == 0 or i == steps:
            conds.append(core == (1 if i == 0 else 0))
        if extra is not None:
            conds.append(extra)
        return functools.reduce(jnp.logical_and, conds) if conds else None

    def run_if(cond, fn):
        if cond is None:
            fn()
        else:
            pl.when(cond)(fn)

    def ring_start(i):
        run_if(here(i), lambda: ring_send(i).start())

    def row_start(i):
        for dx in range(1, nx):
            run_if(here(i, xpos + dx < nx), lambda: row_send(dx, i).start())

    ring_start(1)
    row_start(0)

    before = pbuf[member, 1]
    one_back = pbuf[jnp.maximum(member - 1, 0), 1]
    two_back = pbuf[jnp.maximum(member - 2, 0), 1]
    ext2 = lead & (member >= 2)
    ext3 = lead & (member == 3)

    def extra_tail(r0, c0):
        value2 = one_back[r0 : r0 + 1] + one_back[r0 + 1 : r0 + 2]
        value3 = two_back[r0 : r0 + 1] + two_back[r0 + 1 : r0 + 2]
        return jnp.where(ext2, value2, 0.0) + jnp.where(ext3, value3, 0.0)

    extra_count = jnp.where(ext2, one_back[4:5, 4:5] + one_back[4:5, 5:6], 0.0) + jnp.where(
        ext3, two_back[4:5, 4:5] + two_back[4:5, 5:6], 0.0
    )
    prev_count = before[4:5, 5:6]
    early_count = before[4:5, 4:5] + extra_count
    late_count = early_count + prev_count
    early_size = jnp.maximum(early_count, 1.0)
    late_size = jnp.maximum(late_count, 1.0)
    early_key = before[0:1] + extra_tail(0, 0)
    late_key = (early_key + before[1:2]) / late_size
    early_key = early_key / early_size
    early_value = before[2:3] + extra_tail(2, 0)
    late_value = (early_value + before[3:4]) / late_size
    early_value = early_value / early_size
    rw = iota((16, width), 0)
    run_keys = jnp.where(rw == 0, early_key, jnp.where(rw == 1, late_key, 0.0))
    run_hi = run_keys.astype(BF16)
    run_lo = (run_keys - run_hi.astype(F32)).astype(BF16)
    run_values = jnp.where(rw == 0, early_value, jnp.where(rw == 1, late_value, 0.0))
    ekh[0:16, :] = own_keys
    ekh[16:32, :] = run_hi
    ekh[32:, :] = jnp.zeros((HD - 32, width), BF16)
    ekl[0:16, :] = jnp.zeros((16, width), BF16)
    ekl[16:32, :] = run_lo
    ekl[32:, :] = jnp.zeros((HD - 32, width), BF16)
    evv[0:16, :] = own_values
    evv[16:32, :] = run_values.astype(BF16)
    evv[32:, :] = jnp.zeros((HD - 32, width), BF16)

    own_row = jnp.sum(jnp.where(l16 == r16, own_bias, 0.0), axis=0, keepdims=True)
    early_bias = jnp.where(early_count > 0.5, jnp.log(early_size) * (1.0 / SCALE), NEG)
    late_bias = jnp.where(late_count > 0.5, jnp.log(late_size) * (1.0 / SCALE), NEG)
    el = iota((half, HD), 1)
    owner = lax.div(el, 4)
    for b in range(2):
        mine = columns[b * half : (b + 1) * half]
        visible = (el < 16) & (
            (owner < member) | ((owner == member) & (lax.rem(el, 4).astype(F32) < mine))
        )
        run_bias = early_bias if b == 0 else late_bias
        run_ok = (el == 16 + b) & (mine == 0.0)
        maskb[b, :, tok:] = jnp.where(visible, own_row, jnp.where(run_ok, run_bias, NEG))
    wide_first = jnp.concatenate([columns[:half]] * (half // HD), axis=1)
    halo_ok = (wide_first == 0.0) & (iota((half, half), 1).astype(F32) >= half - prev_count)
    maskb[0, :, 0:half] = jnp.where(halo_ok, 0.0, NEG)

    ones_tok = jnp.ones((tok, HD), BF16)
    ones_ext = jnp.ones((HD, HD), BF16)

    def window(hs, b):
        lo = half
        count = half * (b + 1)
        rows = slice(b * half, (b + 1) * half)
        lanes = [pl.ds(pl.multiple_of(h * HD, HD), HD) for h in hs]
        scores = []
        for ln in lanes:
            q = qd[rows, ln]
            ext = jnp.concatenate([ekh[:, ln], ekl[:, ln]], axis=1)
            scores.append(
                jnp.concatenate(
                    [dot_nt(q, kx[lo : lo + count, ln]),
                     dot_nt(jnp.concatenate([q, q], axis=1), ext)], axis=1,
                ) + maskb[b, :, tok - count :]
            )
        tops = [jnp.max(s, axis=1, keepdims=True) for s in scores]
        probs = [jnp.exp2((s - m) * EXP_SCALE).astype(BF16) for s, m in zip(scores, tops)]
        for h, ln, p, m in zip(hs, lanes, probs, tops):
            v = jnp.concatenate([vx[lo : lo + count, ln], ones_tok[:count]], axis=1)
            ev = jnp.concatenate([evv[:, ln], ones_ext], axis=1)
            acc[h, rows, :] = dot(p[:, :count], v) + dot(p[:, count:], ev)
            mrow[h, rows, :] = jnp.broadcast_to(m, (half, HD))

    def windows(lo, hi, b):
        def body(n, _):
            window((2 * n, 2 * n + 1), b)
            return 0

        lax.fori_loop(lo // 2, hi // 2, body, 0)

    share = heads // steps

    def landed(i):
        def go():
            ring_recv(i).wait_recv()
            if i < steps:
                ring_start(i + 1)

        run_if(here(i), go)
        row_start(i)
        run_if(here(i), lambda: pass_on(0, i).start())

    def rows_landed(i):
        for dx in range(1, nx):
            def go():
                row_recv(dx, i).wait_recv()
                pass_on(dx, i).start()

            run_if(here(i, xpos >= dx), go)

    windows(0, heads // 2, 1)
    for i in range(1, steps + 1):
        landed(i)
        if i == 1:
            windows(heads // 2, heads, 1)
        elif i == 2:
            windows(0, heads // 2, 0)
        elif i == 3:
            windows(heads // 2, heads, 0)
    for i in range(0, steps + 1):
        rows_landed(i)

    @pl.when(d > 0)
    def _():
        halo_copy(0, kx).wait_recv()
        halo_copy(1, vx).wait_recv()

    for dx in range(nx):
        for i in range(0 if dx else 1, steps + 1):
            run_if(
                there(i, (xpos >= dx) if dx else None),
                lambda: passed(dx, i).wait_recv(),
            )

    nkeys = ngroups * 16
    flat_aux = tab[:, :, 2 * width :].reshape(nkeys, HD)
    key_group = lax.div(iota((nkeys, HD), 0), 16)
    off = jnp.where(iota((nkeys, HD), 1) == 0, NEG, 0.0)
    kaux[...] = jnp.where(key_group < group, flat_aux.astype(F32), off).astype(BF16)
    squares[...] = jnp.zeros(squares.shape, F32)
    ones_key = jnp.ones((nkeys, HD), BF16)

    def landmarks(h, _):
        lanes = pl.ds(pl.multiple_of(h * HD, HD), HD)
        vlanes = pl.ds(pl.multiple_of(width + h * HD, HD), HD)
        keys = jnp.concatenate([tab[:, :, lanes].reshape(nkeys, HD), kaux[...]], axis=1)
        values = jnp.concatenate([tab[:, :, vlanes].reshape(nkeys, HD), ones_key], axis=1)
        halo_values = jnp.concatenate([vx[0:half, lanes], ones_tok[:half]], axis=1)
        blocks = [slice(b * half, (b + 1) * half) for b in range(2)]
        scores = [
            dot_nt(jnp.concatenate([qd[rows, lanes], qaux[...]], axis=1), keys)
            for rows in blocks
        ]
        near = dot_nt(qd[0:half, lanes], kx[0:half, lanes]) + maskb[0, :, 0:half]
        tops = [jnp.max(s, axis=1, keepdims=True) for s in scores]
        tops[0] = jnp.maximum(tops[0], jnp.max(near, axis=1, keepdims=True))
        olds = [mrow[h, rows, :] for rows in blocks]
        tops = [jnp.maximum(old, m) for old, m in zip(olds, tops)]
        fades = [jnp.exp2((old - m) * EXP_SCALE) for old, m in zip(olds, tops)]
        probs = [
            jnp.exp2((s - jnp.concatenate([m] * (nkeys // HD), axis=1)) * EXP_SCALE).astype(BF16)
            for s, m in zip(scores, tops)
        ]
        near = jnp.exp2(
            (near - jnp.concatenate([tops[0]] * (half // HD), axis=1)) * EXP_SCALE
        ).astype(BF16)
        sums = [dot(p, values) for p in probs]
        sums[0] = sums[0] + dot(near, halo_values)
        for rows, fade, o in zip(blocks, fades, sums):
            prior = acc[h, rows, :]
            top = prior[:, :HD] * fade + o[:, :HD]
            bottom = prior[:, HD:] * fade + o[:, HD:]
            a = top / bottom
            acc[h, rows, 0:HD] = a
            squares[rows, :] += a * a
        return 0

    lax.fori_loop(0, heads, landmarks, 0)

    ssbuf[0] = jnp.broadcast_to(jnp.sum(squares[...].T, axis=0, keepdims=True), (8, tok))

    def square_copy(n):
        return pltpu.make_async_remote_copy(
            src_ref=ssbuf.at[0], dst_ref=ssbuf.at[n + 1], send_sem=ys.at[n],
            recv_sem=yr.at[n], device_id={"head": ypeers[n]}, device_id_type=MESH,
        )

    for n in range(ny - 1):
        square_copy(n).start()
    for n in range(ny - 1):
        square_copy(n).wait_recv()
    total = ssbuf[0, 0:1]
    for n in range(1, ny):
        total = total + ssbuf[n, 0:1]
    norm = lax.rsqrt(total / (heads * ny * HD) + EPS)
    norm = jnp.broadcast_to(norm, (HD, tok)).T
    for h in range(heads):
        out_ref[:, h * HD : (h + 1) * HD] = (
            acc[h, :, 0:HD] * norm
        ).astype(BF16)

    for copy in sends:
        copy.wait_send()

    @pl.when(sends_on)
    def _():
        for n in range(4):
            tail_copy(n).wait_send()

    @pl.when(d < ndev - 1)
    def _():
        halo_copy(0, kx).wait_send()
        halo_copy(1, vx).wait_send()

    for i in range(1, steps + 1):
        run_if(here(i), lambda: ring_send(i).wait_send())
    for i in range(0, steps + 1):
        for dx in range(1, nx):
            run_if(here(i, xpos + dx < nx), lambda: row_send(dx, i).wait_send())
        for dx in range(nx):
            if dx or i:
                run_if(
                    here(i, (xpos >= dx) if dx else None),
                    lambda: pass_on(dx, i).wait_send(),
                )
    for n in range(ny - 1):
        square_copy(n).wait_send()


def solution(mesh, nx=NX, nz=NZ):
    ny = mesh.shape["head"]

    def on_device(q_raw, k_raw, v_raw, block_scales, segment_ids, norm_gain):
        tok, width = q_raw.shape
        heads = width // HD
        half = tok // 2
        groups = nx * nz // 2
        steps = nz // 4
        dma = pltpu.SemaphoreType.DMA
        hbm = pl.BlockSpec(memory_space=pl.ANY)
        vmem = pl.BlockSpec(memory_space=pltpu.VMEM)
        smem = pl.BlockSpec(memory_space=pltpu.SMEM)
        out = pl.pallas_call(
            functools.partial(kernel, (nx, nz, ny)),
            out_shape=jax.ShapeDtypeStruct((tok, width), BF16),
            in_specs=[hbm, hbm, hbm, smem, vmem],
            out_specs=vmem,
            scratch_shapes=[
                pltpu.VMEM((tok, width), BF16),
                pltpu.VMEM((tok, width), BF16),
                pltpu.VMEM((tok, width), BF16),
                pltpu.VMEM((tok, width), BF16),
                pltpu.VMEM((tok + half, width), BF16),
                pltpu.VMEM((tok + half, width), BF16),
                pltpu.VMEM((2, 8, width), F32),
                pltpu.VMEM((5, 2, 8, width), F32),
                pltpu.VMEM((8, width), F32),
                pltpu.VMEM((16, width), F32),
                pltpu.VMEM((16, width), F32),
                pltpu.VMEM((groups, 16, 2 * width + HD), BF16),
                pltpu.VMEM((groups * 16, HD), BF16),
                pltpu.VMEM((half, HD), BF16),
                pltpu.VMEM((HD, width), BF16),
                pltpu.VMEM((HD, width), BF16),
                pltpu.VMEM((HD, width), BF16),
                pltpu.VMEM((16, HD), F32),
                pltpu.VMEM((2, half, tok + HD), F32),
                pltpu.VMEM((heads, tok, 2 * HD), F32),
                pltpu.VMEM((heads, tok, HD), F32),
                pltpu.VMEM((tok, HD), F32),
                pltpu.VMEM((ny, 8, tok), F32),
                dma((3,)), dma((2,)), dma((2,)), dma((7,)), dma((5,)),
                dma((steps,)), dma((steps,)),
                dma((nx - 1, steps + 1)), dma((nx - 1, steps + 1)),
                dma((nx, steps + 1)), dma((nx, steps + 1)),
                dma((max(ny - 1, 1),)), dma((max(ny - 1, 1),)),
            ],
            compiler_params=pltpu.CompilerParams(
                collective_id=0, has_side_effects=True, vmem_limit_bytes=60000000
            ),
            name="attention",
        )(
            q_raw, k_raw, v_raw, block_scales,
            segment_ids.reshape(1, tok),
        )
        return (out.astype(F32) * norm_gain[None, :]).astype(BF16)

    in_specs = (
        P("seq", "head"),
        P("seq", "head"),
        P("seq", "head"),
        P(None, "seq", "head"),
        P("seq"),
        P("head"),
    )
    return jax.shard_map(
        on_device, mesh=mesh, in_specs=in_specs, out_specs=P("seq", "head"), check_vma=False
    )
```

```python
import functools
import jax
import jax.numpy as jnp
from jax import lax
from jax.experimental import pallas as pl
from jax.experimental.pallas import tpu as pltpu
from jax.sharding import PartitionSpec as P

HEADS = 32
HD = 128
CAP = 4
BLK = 128
SCALE = 1.0 / HD**0.5
LOG2E = 1.4426950408889634
EXP_SCALE = SCALE * LOG2E
NEG = -1e30
EPS = 1e-6
NX, NZ, NC = 4, 16, 2
MESH = pl.DeviceIdType.MESH
F32 = jnp.float32
BF16 = jnp.bfloat16
NT = (((1,), (1,)), ((), ()))


def dot(a, b):
    return jnp.dot(a, b, preferred_element_type=F32)


def dot_nt(a, b):
    return lax.dot_general(a, b, NT, preferred_element_type=F32)


def iota(shape, dim):
    return lax.broadcasted_iota(jnp.int32, shape, dim)


def kernel(
    dims,
    q_hbm, k_hbm, v_hbm, scales, seg_ref,
    out_ref,
    raw_q, raw_k, raw_v, qd, kx, vx,
    packet, pbuf, lmk, lkf, lvf, tab, kaux, qaux, ekh, ekl, evv, lbias,
    maskb, acc, mrow, squares, ssbuf,
    in_sem, halo_s, halo_r, ps, pr, zs, zr, xs, xr, ds, dr, ys, yr,
):
    nx, nz, ny = dims
    pairs = nz // 2
    ndev = nx * nz * NC
    tok, width = out_ref.shape
    half = tok // 2
    heads = width // HD
    d = lax.axis_index("seq")
    y = lax.axis_index("head")
    core = lax.rem(d, 2)
    zpos = lax.rem(lax.div(d, 2), nz)
    xpos = lax.div(d, 2 * nz)
    pair = lax.div(zpos, 2)
    group = lax.div(d, 4)
    ngroups = ndev // 4
    member = lax.rem(d, 4)
    sgn = 1 - 2 * core
    partner = d + sgn

    def at(x, z, c):
        return (x * nz + z) * 2 + c

    loads = [
        pltpu.make_async_copy(src, dst, in_sem.at[n])
        for n, (src, dst) in enumerate(((k_hbm, raw_k), (v_hbm, raw_v), (q_hbm, raw_q)))
    ]
    for load in loads:
        load.start()

    znext = lax.rem(zpos + 2 * sgn + nz, nz)
    zprev = lax.rem(zpos - 2 * sgn + nz, nz)
    peers = [group * 4 + lax.rem(member + n, 4) for n in (1, 2, 3)]
    nextg = [lax.rem(group + 1, ngroups) * 4 + n for n in range(4)]
    prevg = [lax.rem(group + ngroups - 1, ngroups) * 4 + n for n in range(4)]
    xpeers = [at(lax.rem(xpos + n, nx), zpos, core) for n in range(1, nx)]
    zpeers = [at(xpos, znext, core), at(xpos, zprev, core)]
    ypeers = [lax.rem(y + n, ny) for n in range(1, ny)]
    for r in range(1, nx):
        @pl.when(xpos < r)
        def _():
            for o in range(pairs):
                tab[o * nx + r] = jnp.zeros((16, tab.shape[2]), BF16)

    barrier = pltpu.get_barrier_semaphore()
    greeted = peers + nextg + prevg + xpeers + zpeers
    for peer in greeted:
        pl.semaphore_signal(barrier, inc=1, device_id={"seq": peer}, device_id_type=MESH)
    for peer in ypeers:
        pl.semaphore_signal(barrier, inc=1, device_id={"head": peer}, device_id_type=MESH)

    seg = seg_ref[...]
    first = jnp.min(seg, axis=1, keepdims=True)
    last = jnp.max(seg, axis=1, keepdims=True)
    end = last - first
    local = seg - first
    endf = end.astype(F32)
    row = iota((16, tok), 0)
    pos = iota((16, tok), 1)
    slot = lax.rem(row, 4)
    wide = jnp.broadcast_to(local, (16, tok))
    is_slot = (row < 8) & (wide == slot) & (slot < end)
    is_tail = (row >= 8) & (wide == end) & (lax.rem(row, 2) == lax.div(pos, half))
    pick32 = jnp.where(is_slot | is_tail, 1.0, 0.0)
    pick = pick32.astype(BF16)
    counts = jnp.sum(pick32, axis=1, keepdims=True)
    r16 = iota((16, HD), 0)
    l16 = iota((16, HD), 1)
    want = jnp.where(r16 < 4, r16, jnp.where((r16 >= 8) & (r16 < 10), r16 - 4, -1))
    count_row = jnp.sum(jnp.where(l16 == want, counts, 0.0), axis=0, keepdims=True)
    lane = iota((1, HD), 1)
    count_row = jnp.where(lane == 6, endf, count_row)
    count_wide = jnp.concatenate([count_row] + [jnp.zeros((1, HD), F32)] * (heads - 1), axis=1)

    def dequantize(src, which, dst, base):
        def block(b, _):
            for h in range(heads):
                factor = scales[which, b, h]
                rows = pl.ds(pl.multiple_of(b * BLK, BLK), BLK)
                piece = src[rows, h * HD : (h + 1) * HD].astype(F32) * factor
                dst[pl.ds(pl.multiple_of(base + b * BLK, BLK), BLK), h * HD : (h + 1) * HD] = (
                    piece.astype(BF16)
                )
            return 0

        lax.fori_loop(0, tok // BLK, block, 0)

    loads[0].wait()
    dequantize(raw_k, 1, kx, half)
    key_sums = dot(pick, kx[half:, :])
    loads[1].wait()
    dequantize(raw_v, 2, vx, half)
    value_sums = dot(pick, vx[half:, :])
    r8 = iota((8, width), 0)
    packet[0] = jnp.where(r8 < 4, key_sums[0:8], value_sums[0:8])
    packet[1] = jnp.where(
        r8 < 2, key_sums[8:16], jnp.where(r8 == 4, count_wide, value_sums[8:16])
    )

    pl.semaphore_wait(barrier, len(greeted) + len(ypeers))

    sends = []
    for n, peer in enumerate(peers):
        sends.append(
            pltpu.make_async_remote_copy(
                src_ref=packet, dst_ref=pbuf.at[1 + member], send_sem=ps.at[n],
                recv_sem=pr.at[1 + member], device_id={"seq": peer}, device_id_type=MESH,
            )
        )
    for copy in sends:
        copy.start()

    def tail_copy(n):
        return pltpu.make_async_remote_copy(
            src_ref=packet.at[1], dst_ref=pbuf.at[0, 1], send_sem=ps.at[3 + n],
            recv_sem=pr.at[0], device_id={"seq": nextg[n]}, device_id_type=MESH,
        )

    sends_on = (member == 3) & (group < ngroups - 1)

    @pl.when(sends_on)
    def _():
        for n in range(4):
            tail_copy(n).start()

    follower = lax.rem(d + 1, ndev)

    def halo_copy(n, ref):
        return pltpu.make_async_remote_copy(
            src_ref=ref.at[pl.ds(tok, half)], dst_ref=ref.at[pl.ds(0, half)],
            send_sem=halo_s.at[n], recv_sem=halo_r.at[n],
            device_id={"seq": follower}, device_id_type=MESH,
        )

    @pl.when(d < ndev - 1)
    def _():
        halo_copy(0, kx).start()
        halo_copy(1, vx).start()

    @pl.when(d == 0)
    def _():
        kx[0:half, :] = jnp.zeros((half, width), BF16)
        vx[0:half, :] = jnp.zeros((half, width), BF16)

    @pl.when(group == 0)
    def _():
        pbuf[0, 1] = jnp.zeros((8, width), F32)

    columns = jnp.broadcast_to(local.astype(F32), (HD, tok)).T
    own_ids = local.astype(F32)
    for b in range(2):
        mine = columns[b * half : (b + 1) * half]
        width_b = half * (b + 1)
        wide_mine = jnp.concatenate([mine] * (width_b // HD), axis=1)
        i_pos = iota((half, width_b), 0) + b * half
        ok = (wide_mine == own_ids[:, :width_b]) & (iota((half, width_b), 1) <= i_pos)
        start = half * (1 - b)
        maskb[b, :, start:tok] = jnp.where(ok, 0.0, NEG)
    qaux[...] = jnp.where(iota((half, HD), 1) < 3, 1.0, 0.0).astype(BF16)
    loads[2].wait()
    dequantize(raw_q, 0, qd, 0)

    pbuf[1 + member] = packet[...]
    for n in (1, 2, 3):
        other = lax.rem(member + n, 4)
        pltpu.make_async_remote_copy(
            src_ref=packet, dst_ref=pbuf.at[1 + other], send_sem=ps.at[0],
            recv_sem=pr.at[1 + other], device_id={"seq": peers[0]}, device_id_type=MESH,
        ).wait_recv()

    @pl.when(group > 0)
    def _():
        tail_copy(0).wait_recv()

    lead = group == 0
    r8n = iota((8, HD), 0)
    l8n = iota((8, HD), 1)
    tails = [pbuf[n, 1] for n in range(5)]

    def whole_tail(t):
        return t[0:1] + t[1:2], t[2:3] + t[3:4], t[4:5, 4:5] + t[4:5, 5:6]

    for j in range(4):
        key_tail, value_tail, tail_count = whole_tail(tails[j])
        for back in range(1, j):
            extra = whole_tail(tails[j - back])
            key_tail = key_tail + jnp.where(lead, extra[0], 0.0)
            value_tail = value_tail + jnp.where(lead, extra[1], 0.0)
            tail_count = tail_count + jnp.where(lead, extra[2], 0.0)
        total = pbuf[1 + j, 0]
        total = total + jnp.where(r8 == 0, key_tail, jnp.where(r8 == 4, value_tail, 0.0))
        crow = tails[j + 1][4:5, 0:HD]
        slot8 = lax.rem(r8n, 4)
        number = jnp.sum(jnp.where(l8n == slot8, crow, 0.0), axis=1, keepdims=True)
        rc = iota((8, 1), 0)
        number = number + jnp.where(lax.rem(rc, 4) == 0, tail_count, 0.0)
        number = jnp.maximum(number, 1.0)
        done = (lax.rem(rc, 4)).astype(F32) < crow[0:1, 6:7]
        value = total / number
        lmk[...] = value
        lkf[4 * j : 4 * j + 4, :] = lmk[0:4, :]
        lvf[4 * j : 4 * j + 4, :] = lmk[4:8, :]
        bias = jnp.where(done, jnp.log(number) * (1.0 / SCALE), NEG)
        lbias[4 * j : 4 * j + 4, :] = jnp.broadcast_to(bias, (8, HD))[0:4]

    own_bias = lbias[...]
    hi = own_bias.astype(BF16).astype(F32)
    mid = (own_bias - hi).astype(BF16).astype(F32)
    low = own_bias - hi - mid
    aux = jnp.where(l16 == 0, hi, jnp.where(l16 == 1, mid, jnp.where(l16 == 2, low, 0.0)))
    own_keys = lkf[...].astype(BF16)
    own_values = lvf[...].astype(BF16)
    tab[xpos, :, 0:width] = own_keys
    tab[xpos, :, width : 2 * width] = own_values
    tab[xpos, :, 2 * width :] = aux.astype(BF16)

    steps = pairs // 2

    def place(row_x, i, c):
        if i == 0 or i == steps:
            return max(2 * i - 1, 0) * nx + row_x
        return (2 * i - 1 + c) * nx + row_x

    def chunk_copy(source, dest, send_sem, recv_sem, target):
        return pltpu.make_async_remote_copy(
            src_ref=tab.at[source], dst_ref=tab.at[dest], send_sem=send_sem,
            recv_sem=recv_sem, device_id={"seq": target}, device_id_type=MESH,
        )

    def ring_send(i):
        return chunk_copy(place(xpos, i - 1, core), place(xpos, i, core), zs.at[i - 1],
                          zr.at[i - 1], at(xpos, znext, core))

    ring_recv = ring_send

    own_edges = ((0, 0, 1, None), (1, 1, 0, 1), (1, 1, 2, None), (0, 0, 3, None), (2, 2, 3, None))
    relay_edges = ((1, 0, 2, 0), (2, 1, 3, 0), (3, 0, 2, 1), (0, 1, 3, 1))
    far_edges = ((0, 0, 2, None), (1, 1, 3, None))
    direct_from = steps - 1

    def owned(i):
        if i < direct_from:
            return own_edges
        return tuple(e for e in own_edges if e != (1, 1, 0, 1)) + far_edges

    def relayed(i):
        return relay_edges if i < direct_from else ()

    def edge_copy(edge, i):
        _, r, to, _ = edge
        n = (to - r) % nx - 1
        n_slot = place(r, i, core)
        return chunk_copy(n_slot, n_slot, xs.at[n, i], xr.at[n, i], at(to, zpos, core))

    def edge_if(edge, i, end, fn):
        cond = xpos == edge[end]
        if edge[3] is not None:
            if (i == 0 and edge[3] == 1) or (i == steps and edge[3] == 0):
                return
            cond = cond & (core == edge[3])
        run_if(here(i, cond), fn)

    def pass_on(dx, i):
        n_slot = place(xpos - dx, i, core)
        return chunk_copy(n_slot, n_slot, ds.at[dx, i], dr.at[dx, i], partner)

    def passed(dx, i):
        n_slot = place(xpos - dx, i, 1 - core)
        return chunk_copy(n_slot, n_slot, ds.at[dx, i], dr.at[dx, i], partner)

    def here(i, extra=None):
        conds = []
        if i == 0 or i == steps:
            conds.append(core == (0 if i == 0 else 1))
        if extra is not None:
            conds.append(extra)
        return functools.reduce(jnp.logical_and, conds) if conds else None

    def there(i, extra=None):
        conds = []
        if i == 0 or i == steps:
            conds.append(core == (1 if i == 0 else 0))
        if extra is not None:
            conds.append(extra)
        return functools.reduce(jnp.logical_and, conds) if conds else None

    def run_if(cond, fn):
        if cond is None:
            fn()
        else:
            pl.when(cond)(fn)

    def ring_start(i):
        run_if(here(i), lambda: ring_send(i).start())

    def row_start(i):
        for edge in owned(i):
            edge_if(edge, i, 0, lambda: edge_copy(edge, i).start())

    ring_start(1)
    row_start(0)

    before = pbuf[member, 1]
    one_back = pbuf[jnp.maximum(member - 1, 0), 1]
    two_back = pbuf[jnp.maximum(member - 2, 0), 1]
    ext2 = lead & (member >= 2)
    ext3 = lead & (member == 3)

    def extra_tail(r0, c0):
        value2 = one_back[r0 : r0 + 1] + one_back[r0 + 1 : r0 + 2]
        value3 = two_back[r0 : r0 + 1] + two_back[r0 + 1 : r0 + 2]
        return jnp.where(ext2, value2, 0.0) + jnp.where(ext3, value3, 0.0)

    extra_count = jnp.where(ext2, one_back[4:5, 4:5] + one_back[4:5, 5:6], 0.0) + jnp.where(
        ext3, two_back[4:5, 4:5] + two_back[4:5, 5:6], 0.0
    )
    prev_count = before[4:5, 5:6]
    early_count = before[4:5, 4:5] + extra_count
    late_count = early_count + prev_count
    early_size = jnp.maximum(early_count, 1.0)
    late_size = jnp.maximum(late_count, 1.0)
    early_key = before[0:1] + extra_tail(0, 0)
    late_key = (early_key + before[1:2]) / late_size
    early_key = early_key / early_size
    early_value = before[2:3] + extra_tail(2, 0)
    late_value = (early_value + before[3:4]) / late_size
    early_value = early_value / early_size
    rw = iota((16, width), 0)
    run_keys = jnp.where(rw == 0, early_key, jnp.where(rw == 1, late_key, 0.0))
    run_hi = run_keys.astype(BF16)
    run_lo = (run_keys - run_hi.astype(F32)).astype(BF16)
    run_values = jnp.where(rw == 0, early_value, jnp.where(rw == 1, late_value, 0.0))
    ekh[0:16, :] = own_keys
    ekh[16:32, :] = run_hi
    ekh[32:, :] = jnp.zeros((HD - 32, width), BF16)
    ekl[0:16, :] = jnp.zeros((16, width), BF16)
    ekl[16:32, :] = run_lo
    ekl[32:, :] = jnp.zeros((HD - 32, width), BF16)
    evv[0:16, :] = own_values
    evv[16:32, :] = run_values.astype(BF16)
    evv[32:, :] = jnp.zeros((HD - 32, width), BF16)

    own_row = jnp.sum(jnp.where(l16 == r16, own_bias, 0.0), axis=0, keepdims=True)
    early_bias = jnp.where(early_count > 0.5, jnp.log(early_size) * (1.0 / SCALE), NEG)
    late_bias = jnp.where(late_count > 0.5, jnp.log(late_size) * (1.0 / SCALE), NEG)
    el = iota((half, HD), 1)
    owner = lax.div(el, 4)
    for b in range(2):
        mine = columns[b * half : (b + 1) * half]
        visible = (el < 16) & (
            (owner < member) | ((owner == member) & (lax.rem(el, 4).astype(F32) < mine))
        )
        run_bias = early_bias if b == 0 else late_bias
        run_ok = (el == 16 + b) & (mine == 0.0)
        maskb[b, :, tok:] = jnp.where(visible, own_row, jnp.where(run_ok, run_bias, NEG))
    wide_first = jnp.concatenate([columns[:half]] * (half // HD), axis=1)
    halo_ok = (wide_first == 0.0) & (iota((half, half), 1).astype(F32) >= half - prev_count)
    maskb[0, :, 0:half] = jnp.where(halo_ok, 0.0, NEG)

    ones_tok = jnp.ones((tok, HD), BF16)
    ones_ext = jnp.ones((HD, HD), BF16)

    def window(hs, b):
        lo = half
        count = half * (b + 1)
        rows = slice(b * half, (b + 1) * half)
        lanes = [pl.ds(pl.multiple_of(h * HD, HD), HD) for h in hs]
        scores = []
        for ln in lanes:
            q = qd[rows, ln]
            ext = jnp.concatenate([ekh[:, ln], ekl[:, ln]], axis=1)
            scores.append(
                jnp.concatenate(
                    [dot_nt(q, kx[lo : lo + count, ln]),
                     dot_nt(jnp.concatenate([q, q], axis=1), ext)], axis=1,
                ) + maskb[b, :, tok - count :]
            )
        tops = [jnp.max(s, axis=1, keepdims=True) for s in scores]
        probs = [jnp.exp2((s - m) * EXP_SCALE).astype(BF16) for s, m in zip(scores, tops)]
        for h, ln, p, m in zip(hs, lanes, probs, tops):
            v = jnp.concatenate([vx[lo : lo + count, ln], ones_tok[:count]], axis=1)
            ev = jnp.concatenate([evv[:, ln], ones_ext], axis=1)
            acc[h, rows, :] = dot(p[:, :count], v) + dot(p[:, count:], ev)
            mrow[h, rows, :] = jnp.broadcast_to(m, (half, HD))

    def windows(lo, hi, b):
        def body(n, _):
            window((2 * n, 2 * n + 1), b)
            return 0

        lax.fori_loop(lo // 2, hi // 2, body, 0)

    share = heads // steps

    def landed(i):
        def go():
            ring_recv(i).wait_recv()
            if i < steps:
                ring_start(i + 1)

        run_if(here(i), go)
        row_start(i)
        run_if(here(i), lambda: pass_on(0, i).start())

    def rows_landed(i, edges):
        for edge in edges:
            def go():
                edge_copy(edge, i).wait_recv()
                if edge[2] > edge[1]:
                    pass_on(edge[2] - edge[1], i).start()

            edge_if(edge, i, 2, go)
            for relay in relayed(i):
                if edge[0] == edge[1] and relay[:2] == (edge[2], edge[1]):
                    edge_if(relay, i, 0, lambda: edge_copy(relay, i).start())

    windows(0, heads // 2, 1)
    for i in range(1, steps + 1):
        landed(i)
        if i == 1:
            windows(heads // 2, heads, 1)
        elif i == 2:
            windows(0, heads // 2, 0)
        elif i == 3:
            windows(heads // 2, heads, 0)
        rows_landed(i - 1, owned(i - 1))
    for i in range(0, direct_from):
        rows_landed(i, relayed(i))

    def passed_wait(i, only=None):
        for dx in range(nx):
            if i == 0 and dx == 0:
                continue
            cond = (xpos >= dx) if dx else None
            if only is not None:
                cond = (core == 1 - only) if cond is None else cond & (core == 1 - only)
            run_if(there(i, cond), lambda: passed(dx, i).wait_recv())

    nkeys = ngroups * 8
    key_slot = lax.div(iota((2 * nkeys, HD), 0), 16)
    order = lax.div(key_slot, nx)
    hop = lax.div(order + 1, 2)
    key_pair = lax.rem(
        jnp.where(lax.rem(order, 2) == 1, pair - hop, pair + hop) + pairs, pairs
    )
    visible_key = lax.rem(key_slot, nx) * pairs + key_pair < group
    off = jnp.where(iota((nkeys, HD), 1) == 0, NEG, 0.0)
    squares[...] = jnp.zeros(squares.shape, F32)
    ones_key = jnp.ones((nkeys, HD), BF16)
    blocks = [slice(b * half, (b + 1) * half) for b in range(2)]

    def mask_part(n):
        flat_aux = tab[n * nkeys // 16 : (n + 1) * nkeys // 16, :, 2 * width :].reshape(nkeys, HD)
        ok = visible_key[n * nkeys : (n + 1) * nkeys]
        kaux[n * nkeys : (n + 1) * nkeys, :] = jnp.where(
            ok, flat_aux.astype(F32), off
        ).astype(BF16)

    def landmarks(h, part):
        lanes = pl.ds(pl.multiple_of(h * HD, HD), HD)
        vlanes = pl.ds(pl.multiple_of(width + h * HD, HD), HD)
        slots = slice(part * nkeys // 16, (part + 1) * nkeys // 16)
        aux_rows = kaux[part * nkeys : (part + 1) * nkeys, :]
        keys = jnp.concatenate([tab[slots, :, lanes].reshape(nkeys, HD), aux_rows], axis=1)
        values = jnp.concatenate([tab[slots, :, vlanes].reshape(nkeys, HD), ones_key], axis=1)
        scores = [
            dot_nt(jnp.concatenate([qd[rows, lanes], qaux[...]], axis=1), keys)
            for rows in blocks
        ]
        values = [values, values]
        if part == 1:
            near = dot_nt(qd[0:half, lanes], kx[0:half, lanes]) + maskb[0, :, 0:half]
            scores[0] = jnp.concatenate([scores[0], near], axis=1)
            near_values = jnp.concatenate([vx[0:half, lanes], ones_tok[:half]], axis=1)
            values[0] = jnp.concatenate([values[0], near_values], axis=0)
        olds = [mrow[h, rows, :] for rows in blocks]
        tops = [
            jnp.maximum(old, jnp.max(s, axis=1, keepdims=True))
            for old, s in zip(olds, scores)
        ]
        fades = [jnp.exp2((old - m) * EXP_SCALE) for old, m in zip(olds, tops)]
        probs = [
            jnp.exp2(
                (s - jnp.concatenate([m] * (s.shape[1] // HD), axis=1)) * EXP_SCALE
            ).astype(BF16)
            for s, m in zip(scores, tops)
        ]
        sums = [dot(p, v) for p, v in zip(probs, values)]
        for rows, fade, m, o in zip(blocks, fades, tops, sums):
            prior = acc[h, rows, :]
            top = prior[:, :HD] * fade + o[:, :HD]
            bottom = prior[:, HD:] * fade + o[:, HD:]
            if part == 0:
                mrow[h, rows, :] = m
                acc[h, rows, 0:HD] = top
                acc[h, rows, HD:] = bottom
            else:
                a = top / bottom
                acc[h, rows, 0:HD] = a
                squares[rows, :] += a * a

    def landmark_pass(part):
        def body(h, _):
            landmarks(h, part)
            return 0

        mask_part(part)
        lax.fori_loop(0, heads, body, 0)

    early = max(steps // 2, 1)
    for i in range(0, early):
        passed_wait(i)
    passed_wait(early, only=0)
    landmark_pass(0)
    rows_landed(steps, owned(steps))
    passed_wait(early, only=1)
    for i in range(early + 1, steps + 1):
        passed_wait(i)

    @pl.when(d > 0)
    def _():
        halo_copy(0, kx).wait_recv()
        halo_copy(1, vx).wait_recv()

    landmark_pass(1)

    ssbuf[0] = jnp.broadcast_to(jnp.sum(squares[...].T, axis=0, keepdims=True), (8, tok))

    def square_copy(n):
        return pltpu.make_async_remote_copy(
            src_ref=ssbuf.at[0], dst_ref=ssbuf.at[n + 1], send_sem=ys.at[n],
            recv_sem=yr.at[n], device_id={"head": ypeers[n]}, device_id_type=MESH,
        )

    for n in range(ny - 1):
        square_copy(n).start()
    for n in range(ny - 1):
        square_copy(n).wait_recv()
    total = ssbuf[0, 0:1]
    for n in range(1, ny):
        total = total + ssbuf[n, 0:1]
    norm = lax.rsqrt(total / (heads * ny * HD) + EPS)
    norm = jnp.broadcast_to(norm, (HD, tok)).T
    for h in range(heads):
        out_ref[:, h * HD : (h + 1) * HD] = (
            acc[h, :, 0:HD] * norm
        ).astype(BF16)

    for copy in sends:
        copy.wait_send()

    @pl.when(sends_on)
    def _():
        for n in range(4):
            tail_copy(n).wait_send()

    @pl.when(d < ndev - 1)
    def _():
        halo_copy(0, kx).wait_send()
        halo_copy(1, vx).wait_send()

    for i in range(1, steps + 1):
        run_if(here(i), lambda: ring_send(i).wait_send())
    for i in range(0, steps + 1):
        for edge in owned(i) + relayed(i):
            edge_if(edge, i, 0, lambda: edge_copy(edge, i).wait_send())
        for dx in range(nx):
            if dx or i:
                run_if(
                    here(i, (xpos >= dx) if dx else None),
                    lambda: pass_on(dx, i).wait_send(),
                )
    for n in range(ny - 1):
        square_copy(n).wait_send()


def solution(mesh, nx=NX, nz=NZ):
    ny = mesh.shape["head"]

    def on_device(q_raw, k_raw, v_raw, block_scales, segment_ids, norm_gain):
        tok, width = q_raw.shape
        heads = width // HD
        half = tok // 2
        groups = nx * nz // 2
        steps = nz // 4
        dma = pltpu.SemaphoreType.DMA
        hbm = pl.BlockSpec(memory_space=pl.ANY)
        vmem = pl.BlockSpec(memory_space=pltpu.VMEM)
        smem = pl.BlockSpec(memory_space=pltpu.SMEM)
        out = pl.pallas_call(
            functools.partial(kernel, (nx, nz, ny)),
            out_shape=jax.ShapeDtypeStruct((tok, width), BF16),
            in_specs=[hbm, hbm, hbm, smem, vmem],
            out_specs=vmem,
            scratch_shapes=[
                pltpu.VMEM((tok, width), BF16),
                pltpu.VMEM((tok, width), BF16),
                pltpu.VMEM((tok, width), BF16),
                pltpu.VMEM((tok, width), BF16),
                pltpu.VMEM((tok + half, width), BF16),
                pltpu.VMEM((tok + half, width), BF16),
                pltpu.VMEM((2, 8, width), F32),
                pltpu.VMEM((5, 2, 8, width), F32),
                pltpu.VMEM((8, width), F32),
                pltpu.VMEM((16, width), F32),
                pltpu.VMEM((16, width), F32),
                pltpu.VMEM((groups, 16, 2 * width + HD), BF16),
                pltpu.VMEM((groups * 16, HD), BF16),
                pltpu.VMEM((half, HD), BF16),
                pltpu.VMEM((HD, width), BF16),
                pltpu.VMEM((HD, width), BF16),
                pltpu.VMEM((HD, width), BF16),
                pltpu.VMEM((16, HD), F32),
                pltpu.VMEM((2, half, tok + HD), F32),
                pltpu.VMEM((heads, tok, 2 * HD), F32),
                pltpu.VMEM((heads, tok, HD), F32),
                pltpu.VMEM((tok, HD), F32),
                pltpu.VMEM((ny, 8, tok), F32),
                dma((3,)), dma((2,)), dma((2,)), dma((7,)), dma((5,)),
                dma((steps,)), dma((steps,)),
                dma((nx - 1, steps + 1)), dma((nx - 1, steps + 1)),
                dma((nx, steps + 1)), dma((nx, steps + 1)),
                dma((max(ny - 1, 1),)), dma((max(ny - 1, 1),)),
            ],
            compiler_params=pltpu.CompilerParams(
                collective_id=0, has_side_effects=True, vmem_limit_bytes=28000000
            ),
            name="attention",
        )(
            *(pltpu.with_memory_space_constraint(a, pltpu.HBM) for a in (q_raw, k_raw, v_raw)),
            block_scales,
            segment_ids.reshape(1, tok),
        )
        return (out.astype(F32) * norm_gain[None, :]).astype(BF16)

    in_specs = (
        P("seq", "head"),
        P("seq", "head"),
        P("seq", "head"),
        P(None, "seq", "head"),
        P("seq"),
        P("head"),
    )
    return jax.shard_map(
        on_device, mesh=mesh, in_specs=in_specs, out_specs=P("seq", "head"), check_vma=False
    )
```

```python
import functools
import jax
import jax.numpy as jnp
from jax import lax
from jax.experimental import pallas as pl
from jax.experimental.pallas import tpu as pltpu
from jax.sharding import PartitionSpec as P

HEADS = 32
HD = 128
CAP = 4
BLK = 128
SCALE = 1.0 / HD**0.5
LOG2E = 1.4426950408889634
EXP_SCALE = SCALE * LOG2E
NEG = -1e30
EPS = 1e-6
NX, NZ, NC = 4, 16, 2
MESH = pl.DeviceIdType.MESH
F32 = jnp.float32
BF16 = jnp.bfloat16
NT = (((1,), (1,)), ((), ()))


def dot(a, b):
    return jnp.dot(a, b, preferred_element_type=F32)


def dot_nt(a, b):
    return lax.dot_general(a, b, NT, preferred_element_type=F32)


def iota(shape, dim):
    return lax.broadcasted_iota(jnp.int32, shape, dim)


def kernel(
    dims,
    q_hbm, k_hbm, v_hbm, scales, seg_ref,
    out_ref,
    raw_q, raw_k, raw_v, qd, kx, vx,
    packet, pbuf, lmk, lkf, lvf, tab, kaux, qaux, ekh, ekl, evv, lbias,
    maskb, acc, mrow, squares, ssbuf,
    in_sem, halo_s, halo_r, ps, pr, zs, zr, xs, xr, ds, dr, ys, yr,
):
    nx, nz, ny = dims
    pairs = nz // 2
    ndev = nx * nz * NC
    tok, width = out_ref.shape
    half = tok // 2
    heads = width // HD
    d = lax.axis_index("seq")
    y = lax.axis_index("head")
    core = lax.rem(d, 2)
    zpos = lax.rem(lax.div(d, 2), nz)
    xpos = lax.div(d, 2 * nz)
    pair = lax.div(zpos, 2)
    group = lax.div(d, 4)
    ngroups = ndev // 4
    member = lax.rem(d, 4)
    sgn = 1 - 2 * core
    partner = d + sgn

    def at(x, z, c):
        return (x * nz + z) * 2 + c

    loads = [
        pltpu.make_async_copy(src, dst, in_sem.at[n])
        for n, (src, dst) in enumerate(((k_hbm, raw_k), (v_hbm, raw_v), (q_hbm, raw_q)))
    ]
    for load in loads:
        load.start()

    znext = lax.rem(zpos + 2 * sgn + nz, nz)
    zprev = lax.rem(zpos - 2 * sgn + nz, nz)
    peers = [group * 4 + lax.rem(member + n, 4) for n in (1, 2, 3)]
    nextg = [lax.rem(group + 1, ngroups) * 4 + n for n in range(4)]
    prevg = [lax.rem(group + ngroups - 1, ngroups) * 4 + n for n in range(4)]
    xpeers = [at(lax.rem(xpos + n, nx), zpos, core) for n in range(1, nx)]
    zpeers = [at(xpos, znext, core), at(xpos, zprev, core)]
    ypeers = [lax.rem(y + n, ny) for n in range(1, ny)]
    for r in range(1, nx):
        @pl.when(xpos < r)
        def _():
            tab[r * pairs : (r + 1) * pairs] = jnp.zeros((pairs, 16, tab.shape[2]), BF16)

    barrier = pltpu.get_barrier_semaphore()
    greeted = peers + nextg + prevg + xpeers + zpeers
    for peer in greeted:
        pl.semaphore_signal(barrier, inc=1, device_id={"seq": peer}, device_id_type=MESH)
    for peer in ypeers:
        pl.semaphore_signal(barrier, inc=1, device_id={"head": peer}, device_id_type=MESH)

    seg = seg_ref[...]
    first = jnp.min(seg, axis=1, keepdims=True)
    last = jnp.max(seg, axis=1, keepdims=True)
    end = last - first
    local = seg - first
    endf = end.astype(F32)
    row = iota((16, tok), 0)
    pos = iota((16, tok), 1)
    slot = lax.rem(row, 4)
    wide = jnp.broadcast_to(local, (16, tok))
    is_slot = (row < 8) & (wide == slot) & (slot < end)
    is_tail = (row >= 8) & (wide == end) & (lax.rem(row, 2) == lax.div(pos, half))
    pick32 = jnp.where(is_slot | is_tail, 1.0, 0.0)
    pick = pick32.astype(BF16)
    counts = jnp.sum(pick32, axis=1, keepdims=True)
    r16 = iota((16, HD), 0)
    l16 = iota((16, HD), 1)
    want = jnp.where(r16 < 4, r16, jnp.where((r16 >= 8) & (r16 < 10), r16 - 4, -1))
    count_row = jnp.sum(jnp.where(l16 == want, counts, 0.0), axis=0, keepdims=True)
    lane = iota((1, HD), 1)
    count_row = jnp.where(lane == 6, endf, count_row)
    count_wide = jnp.concatenate([count_row] + [jnp.zeros((1, HD), F32)] * (heads - 1), axis=1)

    def dequantize(src, which, dst, base):
        def block(b, _):
            for h in range(heads):
                factor = scales[which, b, h]
                rows = pl.ds(pl.multiple_of(b * BLK, BLK), BLK)
                piece = src[rows, h * HD : (h + 1) * HD].astype(F32) * factor
                dst[pl.ds(pl.multiple_of(base + b * BLK, BLK), BLK), h * HD : (h + 1) * HD] = (
                    piece.astype(BF16)
                )
            return 0

        lax.fori_loop(0, tok // BLK, block, 0)

    loads[0].wait()
    dequantize(raw_k, 1, kx, half)
    key_sums = dot(pick, kx[half:, :])
    loads[1].wait()
    dequantize(raw_v, 2, vx, half)
    value_sums = dot(pick, vx[half:, :])
    r8 = iota((8, width), 0)
    packet[0] = jnp.where(r8 < 4, key_sums[0:8], value_sums[0:8])
    packet[1] = jnp.where(
        r8 < 2, key_sums[8:16], jnp.where(r8 == 4, count_wide, value_sums[8:16])
    )

    pl.semaphore_wait(barrier, len(greeted) + len(ypeers))

    sends = []
    for n, peer in enumerate(peers):
        sends.append(
            pltpu.make_async_remote_copy(
                src_ref=packet, dst_ref=pbuf.at[1 + member], send_sem=ps.at[n],
                recv_sem=pr.at[1 + member], device_id={"seq": peer}, device_id_type=MESH,
            )
        )
    for copy in sends:
        copy.start()

    def tail_copy(n):
        return pltpu.make_async_remote_copy(
            src_ref=packet.at[1], dst_ref=pbuf.at[0, 1], send_sem=ps.at[3 + n],
            recv_sem=pr.at[0], device_id={"seq": nextg[n]}, device_id_type=MESH,
        )

    sends_on = (member == 3) & (group < ngroups - 1)

    @pl.when(sends_on)
    def _():
        for n in range(4):
            tail_copy(n).start()

    follower = lax.rem(d + 1, ndev)

    def halo_copy(n, ref):
        return pltpu.make_async_remote_copy(
            src_ref=ref.at[pl.ds(tok, half)], dst_ref=ref.at[pl.ds(0, half)],
            send_sem=halo_s.at[n], recv_sem=halo_r.at[n],
            device_id={"seq": follower}, device_id_type=MESH,
        )

    @pl.when(d < ndev - 1)
    def _():
        halo_copy(0, kx).start()
        halo_copy(1, vx).start()

    @pl.when(d == 0)
    def _():
        kx[0:half, :] = jnp.zeros((half, width), BF16)
        vx[0:half, :] = jnp.zeros((half, width), BF16)

    @pl.when(group == 0)
    def _():
        pbuf[0, 1] = jnp.zeros((8, width), F32)

    columns = jnp.broadcast_to(local.astype(F32), (HD, tok)).T
    own_ids = local.astype(F32)
    for b in range(2):
        mine = columns[b * half : (b + 1) * half]
        width_b = half * (b + 1)
        wide_mine = jnp.concatenate([mine] * (width_b // HD), axis=1)
        i_pos = iota((half, width_b), 0) + b * half
        ok = (wide_mine == own_ids[:, :width_b]) & (iota((half, width_b), 1) <= i_pos)
        start = half * (1 - b)
        maskb[b, :, start:tok] = jnp.where(ok, 0.0, NEG)
    qaux[...] = jnp.where(iota((half, HD), 1) < 3, 1.0, 0.0).astype(BF16)
    loads[2].wait()
    dequantize(raw_q, 0, qd, 0)

    pbuf[1 + member] = packet[...]
    for n in (1, 2, 3):
        other = lax.rem(member + n, 4)
        pltpu.make_async_remote_copy(
            src_ref=packet, dst_ref=pbuf.at[1 + other], send_sem=ps.at[0],
            recv_sem=pr.at[1 + other], device_id={"seq": peers[0]}, device_id_type=MESH,
        ).wait_recv()

    @pl.when(group > 0)
    def _():
        tail_copy(0).wait_recv()

    lead = group == 0
    r8n = iota((8, HD), 0)
    l8n = iota((8, HD), 1)
    tails = [pbuf[n, 1] for n in range(5)]

    def whole_tail(t):
        return t[0:1] + t[1:2], t[2:3] + t[3:4], t[4:5, 4:5] + t[4:5, 5:6]

    for j in range(4):
        key_tail, value_tail, tail_count = whole_tail(tails[j])
        for back in range(1, j):
            extra = whole_tail(tails[j - back])
            key_tail = key_tail + jnp.where(lead, extra[0], 0.0)
            value_tail = value_tail + jnp.where(lead, extra[1], 0.0)
            tail_count = tail_count + jnp.where(lead, extra[2], 0.0)
        total = pbuf[1 + j, 0]
        total = total + jnp.where(r8 == 0, key_tail, jnp.where(r8 == 4, value_tail, 0.0))
        crow = tails[j + 1][4:5, 0:HD]
        slot8 = lax.rem(r8n, 4)
        number = jnp.sum(jnp.where(l8n == slot8, crow, 0.0), axis=1, keepdims=True)
        rc = iota((8, 1), 0)
        number = number + jnp.where(lax.rem(rc, 4) == 0, tail_count, 0.0)
        number = jnp.maximum(number, 1.0)
        done = (lax.rem(rc, 4)).astype(F32) < crow[0:1, 6:7]
        value = total / number
        lmk[...] = value
        lkf[4 * j : 4 * j + 4, :] = lmk[0:4, :]
        lvf[4 * j : 4 * j + 4, :] = lmk[4:8, :]
        bias = jnp.where(done, jnp.log(number) * (1.0 / SCALE), NEG)
        lbias[4 * j : 4 * j + 4, :] = jnp.broadcast_to(bias, (8, HD))[0:4]

    own_bias = lbias[...]
    hi = own_bias.astype(BF16).astype(F32)
    mid = (own_bias - hi).astype(BF16).astype(F32)
    low = own_bias - hi - mid
    aux = jnp.where(l16 == 0, hi, jnp.where(l16 == 1, mid, jnp.where(l16 == 2, low, 0.0)))
    own_keys = lkf[...].astype(BF16)
    own_values = lvf[...].astype(BF16)
    tab[group, :, 0:width] = own_keys
    tab[group, :, width : 2 * width] = own_values
    tab[group, :, 2 * width :] = aux.astype(BF16)

    def chunk_copy(row_x, p, send_sem, recv_sem, target):
        g = row_x * pairs + p
        return pltpu.make_async_remote_copy(
            src_ref=tab.at[g], dst_ref=tab.at[g], send_sem=send_sem, recv_sem=recv_sem,
            device_id={"seq": target}, device_id_type=MESH,
        )

    def ring_pair(i, c_sgn):
        return lax.rem(pair - c_sgn * i + 2 * pairs, pairs)

    steps = pairs // 2

    def ring_send(i):
        return chunk_copy(xpos, ring_pair(i - 1, sgn), zs.at[i - 1], zr.at[i - 1],
                          at(xpos, znext, core))

    def ring_recv(i):
        return chunk_copy(xpos, ring_pair(i, sgn), zs.at[i - 1], zr.at[i - 1],
                          at(xpos, znext, core))

    own_edges = ((0, 0, 1, None), (1, 1, 0, 1), (1, 1, 2, None), (0, 0, 3, None), (2, 2, 3, None))
    relay_edges = ((1, 0, 2, 0), (2, 1, 3, 0), (3, 0, 2, 1), (0, 1, 3, 1))
    far_edges = ((0, 0, 2, None), (1, 1, 3, None))
    direct_from = steps - 1

    def owned(i):
        if i < direct_from:
            return own_edges
        return tuple(e for e in own_edges if e != (1, 1, 0, 1)) + far_edges

    def relayed(i):
        return relay_edges if i < direct_from else ()

    def edge_copy(edge, i):
        _, r, to, _ = edge
        n = (to - r) % nx - 1
        return chunk_copy(r, ring_pair(i, sgn), xs.at[n, i], xr.at[n, i], at(to, zpos, core))

    def edge_if(edge, i, end, fn):
        cond = xpos == edge[end]
        if edge[3] is not None:
            if (i == 0 and edge[3] == 1) or (i == steps and edge[3] == 0):
                return
            cond = cond & (core == edge[3])
        run_if(here(i, cond), fn)

    def pass_on(dx, i):
        return chunk_copy(xpos - dx, ring_pair(i, sgn), ds.at[dx, i], dr.at[dx, i], partner)

    def passed(dx, i):
        return chunk_copy(xpos - dx, ring_pair(i, -sgn), ds.at[dx, i], dr.at[dx, i], partner)

    def here(i, extra=None):
        conds = []
        if i == 0 or i == steps:
            conds.append(core == (0 if i == 0 else 1))
        if extra is not None:
            conds.append(extra)
        return functools.reduce(jnp.logical_and, conds) if conds else None

    def there(i, extra=None):
        conds = []
        if i == 0 or i == steps:
            conds.append(core == (1 if i == 0 else 0))
        if extra is not None:
            conds.append(extra)
        return functools.reduce(jnp.logical_and, conds) if conds else None

    def run_if(cond, fn):
        if cond is None:
            fn()
        else:
            pl.when(cond)(fn)

    def ring_start(i):
        run_if(here(i), lambda: ring_send(i).start())

    def row_start(i):
        for edge in owned(i):
            edge_if(edge, i, 0, lambda: edge_copy(edge, i).start())

    ring_start(1)
    row_start(0)

    before = pbuf[member, 1]
    one_back = pbuf[jnp.maximum(member - 1, 0), 1]
    two_back = pbuf[jnp.maximum(member - 2, 0), 1]
    ext2 = lead & (member >= 2)
    ext3 = lead & (member == 3)

    def extra_tail(r0, c0):
        value2 = one_back[r0 : r0 + 1] + one_back[r0 + 1 : r0 + 2]
        value3 = two_back[r0 : r0 + 1] + two_back[r0 + 1 : r0 + 2]
        return jnp.where(ext2, value2, 0.0) + jnp.where(ext3, value3, 0.0)

    extra_count = jnp.where(ext2, one_back[4:5, 4:5] + one_back[4:5, 5:6], 0.0) + jnp.where(
        ext3, two_back[4:5, 4:5] + two_back[4:5, 5:6], 0.0
    )
    prev_count = before[4:5, 5:6]
    early_count = before[4:5, 4:5] + extra_count
    late_count = early_count + prev_count
    early_size = jnp.maximum(early_count, 1.0)
    late_size = jnp.maximum(late_count, 1.0)
    early_key = before[0:1] + extra_tail(0, 0)
    late_key = (early_key + before[1:2]) / late_size
    early_key = early_key / early_size
    early_value = before[2:3] + extra_tail(2, 0)
    late_value = (early_value + before[3:4]) / late_size
    early_value = early_value / early_size
    rw = iota((16, width), 0)
    run_keys = jnp.where(rw == 0, early_key, jnp.where(rw == 1, late_key, 0.0))
    run_hi = run_keys.astype(BF16)
    run_lo = (run_keys - run_hi.astype(F32)).astype(BF16)
    run_values = jnp.where(rw == 0, early_value, jnp.where(rw == 1, late_value, 0.0))
    ekh[0:16, :] = own_keys
    ekh[16:32, :] = run_hi
    ekh[32:, :] = jnp.zeros((HD - 32, width), BF16)
    ekl[0:16, :] = jnp.zeros((16, width), BF16)
    ekl[16:32, :] = run_lo
    ekl[32:, :] = jnp.zeros((HD - 32, width), BF16)
    evv[0:16, :] = own_values
    evv[16:32, :] = run_values.astype(BF16)
    evv[32:, :] = jnp.zeros((HD - 32, width), BF16)

    own_row = jnp.sum(jnp.where(l16 == r16, own_bias, 0.0), axis=0, keepdims=True)
    early_bias = jnp.where(early_count > 0.5, jnp.log(early_size) * (1.0 / SCALE), NEG)
    late_bias = jnp.where(late_count > 0.5, jnp.log(late_size) * (1.0 / SCALE), NEG)
    el = iota((half, HD), 1)
    owner = lax.div(el, 4)
    for b in range(2):
        mine = columns[b * half : (b + 1) * half]
        visible = (el < 16) & (
            (owner < member) | ((owner == member) & (lax.rem(el, 4).astype(F32) < mine))
        )
        run_bias = early_bias if b == 0 else late_bias
        run_ok = (el == 16 + b) & (mine == 0.0)
        maskb[b, :, tok:] = jnp.where(visible, own_row, jnp.where(run_ok, run_bias, NEG))
    wide_first = jnp.concatenate([columns[:half]] * (half // HD), axis=1)
    halo_ok = (wide_first == 0.0) & (iota((half, half), 1).astype(F32) >= half - prev_count)
    maskb[0, :, 0:half] = jnp.where(halo_ok, 0.0, NEG)

    ones_tok = jnp.ones((tok, HD), BF16)
    ones_ext = jnp.ones((HD, HD), BF16)

    def window(hs, b):
        lo = half
        count = half * (b + 1)
        rows = slice(b * half, (b + 1) * half)
        lanes = [pl.ds(pl.multiple_of(h * HD, HD), HD) for h in hs]
        scores = []
        for ln in lanes:
            q = qd[rows, ln]
            ext = jnp.concatenate([ekh[:, ln], ekl[:, ln]], axis=1)
            scores.append(
                jnp.concatenate(
                    [dot_nt(q, kx[lo : lo + count, ln]),
                     dot_nt(jnp.concatenate([q, q], axis=1), ext)], axis=1,
                ) + maskb[b, :, tok - count :]
            )
        tops = [jnp.max(s, axis=1, keepdims=True) for s in scores]
        probs = [jnp.exp2((s - m) * EXP_SCALE).astype(BF16) for s, m in zip(scores, tops)]
        for h, ln, p, m in zip(hs, lanes, probs, tops):
            v = jnp.concatenate([vx[lo : lo + count, ln], ones_tok[:count]], axis=1)
            ev = jnp.concatenate([evv[:, ln], ones_ext], axis=1)
            acc[h, rows, :] = dot(p[:, :count], v) + dot(p[:, count:], ev)
            mrow[h, rows, :] = jnp.broadcast_to(m, (half, HD))

    def windows(lo, hi, b):
        def body(n, _):
            window((2 * n, 2 * n + 1), b)
            return 0

        lax.fori_loop(lo // 2, hi // 2, body, 0)

    share = heads // steps

    def landed(i):
        def go():
            ring_recv(i).wait_recv()
            if i < steps:
                ring_start(i + 1)

        run_if(here(i), go)
        row_start(i)
        run_if(here(i), lambda: pass_on(0, i).start())

    def rows_landed(i, edges):
        for edge in edges:
            def go():
                edge_copy(edge, i).wait_recv()
                if edge[2] > edge[1]:
                    pass_on(edge[2] - edge[1], i).start()

            edge_if(edge, i, 2, go)
            for relay in relayed(i):
                if edge[0] == edge[1] and relay[:2] == (edge[2], edge[1]):
                    edge_if(relay, i, 0, lambda: edge_copy(relay, i).start())

    windows(0, heads // 2, 1)
    for i in range(1, steps + 1):
        landed(i)
        if i == 1:
            windows(heads // 2, heads, 1)
        elif i == 2:
            windows(0, heads // 2, 0)
        elif i == 3:
            windows(heads // 2, heads, 0)
        rows_landed(i - 1, owned(i - 1))
    for i in range(0, direct_from):
        rows_landed(i, relayed(i))
    rows_landed(steps, owned(steps))

    @pl.when(d > 0)
    def _():
        halo_copy(0, kx).wait_recv()
        halo_copy(1, vx).wait_recv()

    for dx in range(nx):
        for i in range(0 if dx else 1, steps + 1):
            run_if(
                there(i, (xpos >= dx) if dx else None),
                lambda: passed(dx, i).wait_recv(),
            )

    nkeys = ngroups * 16
    flat_aux = tab[:, :, 2 * width :].reshape(nkeys, HD)
    key_group = lax.div(iota((nkeys, HD), 0), 16)
    off = jnp.where(iota((nkeys, HD), 1) == 0, NEG, 0.0)
    kaux[...] = jnp.where(key_group < group, flat_aux.astype(F32), off).astype(BF16)
    squares[...] = jnp.zeros(squares.shape, F32)
    ones_key = jnp.ones((nkeys, HD), BF16)

    def landmarks(h, _):
        lanes = pl.ds(pl.multiple_of(h * HD, HD), HD)
        vlanes = pl.ds(pl.multiple_of(width + h * HD, HD), HD)
        keys = jnp.concatenate([tab[:, :, lanes].reshape(nkeys, HD), kaux[...]], axis=1)
        values = jnp.concatenate([tab[:, :, vlanes].reshape(nkeys, HD), ones_key], axis=1)
        halo_values = jnp.concatenate([vx[0:half, lanes], ones_tok[:half]], axis=1)
        blocks = [slice(b * half, (b + 1) * half) for b in range(2)]
        scores = [
            dot_nt(jnp.concatenate([qd[rows, lanes], qaux[...]], axis=1), keys)
            for rows in blocks
        ]
        near = dot_nt(qd[0:half, lanes], kx[0:half, lanes]) + maskb[0, :, 0:half]
        tops = [jnp.max(s, axis=1, keepdims=True) for s in scores]
        tops[0] = jnp.maximum(tops[0], jnp.max(near, axis=1, keepdims=True))
        olds = [mrow[h, rows, :] for rows in blocks]
        tops = [jnp.maximum(old, m) for old, m in zip(olds, tops)]
        fades = [jnp.exp2((old - m) * EXP_SCALE) for old, m in zip(olds, tops)]
        probs = [
            jnp.exp2((s - jnp.concatenate([m] * (nkeys // HD), axis=1)) * EXP_SCALE).astype(BF16)
            for s, m in zip(scores, tops)
        ]
        near = jnp.exp2(
            (near - jnp.concatenate([tops[0]] * (half // HD), axis=1)) * EXP_SCALE
        ).astype(BF16)
        sums = [dot(p, values) for p in probs]
        sums[0] = sums[0] + dot(near, halo_values)
        for rows, fade, o in zip(blocks, fades, sums):
            prior = acc[h, rows, :]
            top = prior[:, :HD] * fade + o[:, :HD]
            bottom = prior[:, HD:] * fade + o[:, HD:]
            a = top / bottom
            acc[h, rows, 0:HD] = a
            squares[rows, :] += a * a
        return 0

    lax.fori_loop(0, heads, landmarks, 0, unroll=2)

    ssbuf[0] = jnp.broadcast_to(jnp.sum(squares[...].T, axis=0, keepdims=True), (8, tok))

    def square_copy(n):
        return pltpu.make_async_remote_copy(
            src_ref=ssbuf.at[0], dst_ref=ssbuf.at[n + 1], send_sem=ys.at[n],
            recv_sem=yr.at[n], device_id={"head": ypeers[n]}, device_id_type=MESH,
        )

    for n in range(ny - 1):
        square_copy(n).start()
    for n in range(ny - 1):
        square_copy(n).wait_recv()
    total = ssbuf[0, 0:1]
    for n in range(1, ny):
        total = total + ssbuf[n, 0:1]
    norm = lax.rsqrt(total / (heads * ny * HD) + EPS)
    norm = jnp.broadcast_to(norm, (HD, tok)).T
    for h in range(heads):
        out_ref[:, h * HD : (h + 1) * HD] = (
            acc[h, :, 0:HD] * norm
        ).astype(BF16)

    for copy in sends:
        copy.wait_send()

    @pl.when(sends_on)
    def _():
        for n in range(4):
            tail_copy(n).wait_send()

    @pl.when(d < ndev - 1)
    def _():
        halo_copy(0, kx).wait_send()
        halo_copy(1, vx).wait_send()

    for i in range(1, steps + 1):
        run_if(here(i), lambda: ring_send(i).wait_send())
    for i in range(0, steps + 1):
        for edge in owned(i) + relayed(i):
            edge_if(edge, i, 0, lambda: edge_copy(edge, i).wait_send())
        for dx in range(nx):
            if dx or i:
                run_if(
                    here(i, (xpos >= dx) if dx else None),
                    lambda: pass_on(dx, i).wait_send(),
                )
    for n in range(ny - 1):
        square_copy(n).wait_send()


def solution(mesh, nx=NX, nz=NZ):
    ny = mesh.shape["head"]

    def on_device(q_raw, k_raw, v_raw, block_scales, segment_ids, norm_gain):
        tok, width = q_raw.shape
        heads = width // HD
        half = tok // 2
        groups = nx * nz // 2
        steps = nz // 4
        dma = pltpu.SemaphoreType.DMA
        hbm = pl.BlockSpec(memory_space=pl.ANY)
        vmem = pl.BlockSpec(memory_space=pltpu.VMEM)
        smem = pl.BlockSpec(memory_space=pltpu.SMEM)
        out = pl.pallas_call(
            functools.partial(kernel, (nx, nz, ny)),
            out_shape=jax.ShapeDtypeStruct((tok, width), BF16),
            in_specs=[hbm, hbm, hbm, smem, vmem],
            out_specs=vmem,
            scratch_shapes=[
                pltpu.VMEM((tok, width), BF16),
                pltpu.VMEM((tok, width), BF16),
                pltpu.VMEM((tok, width), BF16),
                pltpu.VMEM((tok, width), BF16),
                pltpu.VMEM((tok + half, width), BF16),
                pltpu.VMEM((tok + half, width), BF16),
                pltpu.VMEM((2, 8, width), F32),
                pltpu.VMEM((5, 2, 8, width), F32),
                pltpu.VMEM((8, width), F32),
                pltpu.VMEM((16, width), F32),
                pltpu.VMEM((16, width), F32),
                pltpu.VMEM((groups, 16, 2 * width + HD), BF16),
                pltpu.VMEM((groups * 16, HD), BF16),
                pltpu.VMEM((half, HD), BF16),
                pltpu.VMEM((HD, width), BF16),
                pltpu.VMEM((HD, width), BF16),
                pltpu.VMEM((HD, width), BF16),
                pltpu.VMEM((16, HD), F32),
                pltpu.VMEM((2, half, tok + HD), F32),
                pltpu.VMEM((heads, tok, 2 * HD), F32),
                pltpu.VMEM((heads, tok, HD), F32),
                pltpu.VMEM((tok, HD), F32),
                pltpu.VMEM((ny, 8, tok), F32),
                dma((3,)), dma((2,)), dma((2,)), dma((7,)), dma((5,)),
                dma((steps,)), dma((steps,)),
                dma((nx - 1, steps + 1)), dma((nx - 1, steps + 1)),
                dma((nx, steps + 1)), dma((nx, steps + 1)),
                dma((max(ny - 1, 1),)), dma((max(ny - 1, 1),)),
            ],
            compiler_params=pltpu.CompilerParams(
                collective_id=0, has_side_effects=True, vmem_limit_bytes=28000000
            ),
            name="attention",
        )(
            *(pltpu.with_memory_space_constraint(a, pltpu.HBM) for a in (q_raw, k_raw, v_raw)),
            block_scales,
            segment_ids.reshape(1, tok),
        )
        return (out.astype(F32) * norm_gain[None, :]).astype(BF16)

    in_specs = (
        P("seq", "head"),
        P("seq", "head"),
        P("seq", "head"),
        P(None, "seq", "head"),
        P("seq"),
        P("head"),
    )
    return jax.shard_map(
        on_device, mesh=mesh, in_specs=in_specs, out_specs=P("seq", "head"), check_vma=False
    )
```
